256 devices in a mesh: inl: 8 (over z), xln: 32 (over y, x, core).
Axes of the slice: x: 4, y: 4, z: 8, core: 2. Of those that a mesh axis runs over, the one named last changes fastest.
Arguments:
- noisy: float32 [256, 1024, 512], P('inl', 'xln'), may hold values from -6 to 6
- bound: float32 [256, 1024, 512], P('inl', 'xln'), may hold values from 0.05 to 0.5
Outputs:
- denoised: float32 [256, 1024, 512], P('inl', 'xln')
- dual: float32 [3, 256, 1024, 512], P(None, 'inl', 'xln')
- norms: float32 [2, 2], replicated
The draws below stay inside these ranges and needn't reach their ends.
All inputs are finite; a program needn't handle non-finite values.
Results may differ from the reference program's by a relative error of at most 0.0001.
Values sent between devices are 32-bit elements; how exact they have to be, the bound alone decides.
No kernel may reach another device: no remote copies, remote signals or barrier semaphores. Data moves between devices by JAX's collectives and lax.ppermute only.
A program may use at most 64 MiB of HBM per device.

```python
import math
import jax
import jax.numpy as jnp
from jax import lax

NZ = 512
ITERS = 2
NI = 256
NX = 1024


def levels(key, shape, cuts, least, high):
    def one(position, blocks):
        draws = jax.random.uniform(jax.random.fold_in(jax.random.fold_in(key, 6), position), (blocks,), jnp.float32, least / len(cuts), high / len(cuts))
        return jnp.repeat(jnp.exp(draws), shape[position] // blocks).reshape((-1,) + (1,) * (len(shape) - position - 1))

    gain = one(*cuts[0])
    for cut in cuts[1:]:
        gain = gain * one(*cut)
    return gain


def bell_draw(stream_key, extent, spread, most, split=(), held_as=jnp.bfloat16):
    gain = levels(stream_key, extent, split, -0.22, 0.18) if split else 1.0
    values = jax.random.normal(stream_key, extent, jnp.float32) * spread * gain
    return jnp.minimum(jnp.maximum(values, -most), most).astype(held_as)


def setup_inputs(seed: int = 0) -> dict:
    splits = jax.random.split(jax.random.key(seed), 3)
    return {
        "noisy": bell_draw(splits[0], (NI, NX, NZ), 1.0, 6.0, ((0, 8), (1, 32)), jnp.float32),
        "bound": jnp.clip(jnp.exp(math.log(0.5) - 2.3025851 * jax.random.uniform(splits[1], (NI, NX, NZ), jnp.float32) ** levels(splits[1], (NI, NX, NZ), ((0, 8), (1, 32)), -0.2, 0.2)), 0.05, 0.5),
    }


SIGMA = 0.28
TAU = 0.28

def forward(field, axis):
    first = lax.slice_in_dim(field, 0, 1, axis=axis)
    return jnp.concatenate([jnp.diff(field, axis=axis), jnp.zeros_like(first)], axis=axis)

def backward(field, axis):
    size = field.shape[axis]
    first = lax.slice_in_dim(field, 0, 1, axis=axis)
    earlier = jnp.concatenate([jnp.zeros_like(first), lax.slice_in_dim(field, 0, size - 1, axis=axis)], axis=axis)
    return field - earlier

def reference(noisy, bound):
    primal = noisy
    smooth = noisy
    dual_parts = [jnp.zeros_like(noisy) for axis in range(3)]
    rows = []
    for step in range(ITERS):
        fresh = [jnp.clip(dual_parts[axis] + SIGMA * forward(smooth, axis), -bound, bound) for axis in range(3)]
        diverge = backward(fresh[0], 0) + backward(fresh[1], 1) + backward(fresh[2], 2)
        updated = (primal + TAU * diverge + TAU * noisy) / (1.0 + TAU)
        primal_sum = jnp.sum((updated - primal) ** 2)
        dual_sum = jnp.sum((fresh[0] - dual_parts[0]) ** 2) + jnp.sum((fresh[1] - dual_parts[1]) ** 2) + jnp.sum((fresh[2] - dual_parts[2]) ** 2)
        rows.append(jnp.sqrt(jnp.stack([primal_sum, dual_sum])))
        smooth = 2.0 * updated - primal
        primal = updated
        dual_parts = fresh
    return (primal, jnp.stack(dual_parts), jnp.stack(rows))
```

```python
import jax
import jax.numpy as jnp
from jax import lax
from jax.experimental import pallas as pl
from jax.experimental.pallas import tpu as pltpu
from jax.sharding import PartitionSpec as P

SIGMA = 0.28
TAU = 0.28
C = TAU / (1.0 + TAU)
C_OLD = C / (1.0 + TAU)
TWO_CS = 2.0 * C * SIGMA

LANES = 128
ROWS = 56
OWN = 8
HALO = 40
AXES = ("inl", "xln")
F32 = jnp.float32


def sent_along(value, axis, steps):
    count = lax.axis_size(axis)
    first, last = (max(0, -steps), min(count, count - steps))
    return lax.ppermute(value, axis, [(s, s + steps) for s in range(first, last)])


def clip(value, bound):
    return jnp.minimum(jnp.maximum(value, -bound), bound)


def last_lane():
    return lax.broadcasted_iota(jnp.int32, (8, LANES), 1) == LANES - 1


def first_lane():
    return lax.broadcasted_iota(jnp.int32, (8, LANES), 1) == 0


def depth_next(tiles):
    rolled = [pltpu.roll(t, LANES - 1, 1) for t in tiles] + [tiles[-1]]
    mask = last_lane()
    return [jnp.where(mask, rolled[j + 1], rolled[j]) for j in range(len(tiles))]


def depth_back(tiles):
    rolled = [jnp.zeros((8, LANES), F32)] + [pltpu.roll(t, 1, 1) for t in tiles]
    mask = first_lane()
    return [jnp.where(mask, rolled[j], rolled[j + 1]) for j in range(len(tiles))]


def pack_kernel(n_hbm, b_hbm, f_ref, g_ref, low, high, sems):
    copies = []
    for k, src in enumerate((n_hbm, b_hbm)):
        copies.append(pltpu.make_async_copy(src.at[:, pl.ds(24, 8), :], high.at[k], sems.at[k, 0]))
        copies.append(pltpu.make_async_copy(src.at[:, pl.ds(0, 8), :], low.at[k], sems.at[k, 1]))
    for c in copies:
        c.start()
    for c in copies:
        c.wait()
    depth = n_hbm.shape[2] // LANES

    def body(i, _):
        for k in range(2):
            for j in range(depth):
                lanes = pl.ds(j * LANES, LANES)
                f_ref[i, j, 2 * k : 2 * k + 2, :] = high[k, i, 6:8, lanes]
                g_ref[i, j, 2 * k : 2 * k + 2, :] = low[k, i, 0:2, lanes]
        return 0

    lax.fori_loop(0, n_hbm.shape[0], body, 0)


def pack(noisy, bound):
    ni, _, nz = noisy.shape
    depth = nz // LANES
    message = jax.ShapeDtypeStruct((ni, depth, 4, LANES), F32)
    return pl.pallas_call(
        pack_kernel,
        out_shape=(message, message),
        in_specs=[pl.BlockSpec(memory_space=pl.ANY)] * 2,
        out_specs=[pl.BlockSpec(memory_space=pltpu.VMEM)] * 2,
        scratch_shapes=[
            pltpu.VMEM((2, ni, 8, nz), F32),
            pltpu.VMEM((2, ni, 8, nz), F32),
            pltpu.SemaphoreType.DMA((2, 2)),
        ],
        compiler_params=pltpu.CompilerParams(vmem_limit_bytes=16 << 20),
        name="pack_faces",
    )(noisy, bound)


def fill_columns(p, i, depth, more, f_ref, g_ref, ne, be):
    for j in range(depth):
        ne[p, j, HALO + 6 : HALO + 8, :] = f_ref[i, j, 0:2, :]
        be[p, j, HALO + 6 : HALO + 8, :] = f_ref[i, j, 2:4, :]
        edge = ne[p, j, HALO - 1 : HALO, :]
        ne[p, j, HALO : HALO + 2, :] = g_ref[i, j, 0:2, :]
        be[p, j, HALO : HALO + 2, :] = g_ref[i, j, 2:4, :]
        ne[p, j, HALO : HALO + 1, :] = jnp.where(more, g_ref[i, j, 0:1, :], edge)


def strip(s):
    return pl.ds(OWN + 8 * s, 8)


def strip_next(s):
    return pl.ds(OWN + 8 * s + 1, 8)


def strip_back(s):
    return pl.ds(OWN + 8 * s - 1, 8)


def scale(p, depth, ne, ve, count=5):
    for j in range(depth):
        for s in range(count):
            ve[p, j, strip(s), :] = SIGMA * ne[p, j, strip(s), :]
        ve[p, j, pl.ds(HALO + 8, 1), :] = ve[p, j, pl.ds(OWN, 1), :]


def first_x(p, depth, ve, be, dx, count=5):
    for j in range(depth):
        for s in reversed(range(count)):
            dx[p, j, strip(s), :] = clip(
                ve[p, j, strip_next(s), :] - ve[p, j, strip(s), :], be[p, j, strip(s), :]
            )
        dx[p, j, pl.ds(OWN - 1, 1), :] = dx[p, j, pl.ds(HALO + 7, 1), :]


def cross_divergence(p, s, depth, ve, be, dx):
    v = [ve[p, j, strip(s), :] for j in range(depth)]
    b = [be[p, j, strip(s), :] for j in range(depth)]
    x = [dx[p, j, strip(s), :] for j in range(depth)]
    z = [clip(n - o, k) for n, o, k in zip(depth_next(v), v, b)]
    back = depth_back(z)
    div = [x[j] - dx[p, j, strip_back(s), :] + (z[j] - back[j]) for j in range(depth)]
    return v, b, x, z, div


def planes_kernel(flags, n_hbm, b_hbm, f_ref, g_ref, up_ref, down_ref, ne, be, ve, dx, sems):
    ni, depth = n_hbm.shape[0], n_hbm.shape[2] // LANES
    more_x = flags[1] > 0
    planes = (0, 1, ni - 2, ni - 1)
    copies = []
    for q, i in enumerate(planes):
        for k, (src, dst) in enumerate(((n_hbm, ne), (b_hbm, be))):
            for j in range(depth):
                copies.append(
                    pltpu.make_async_copy(
                        src.at[i, :, pl.ds(j * LANES, LANES)],
                        dst.at[q, j, pl.ds(OWN, 32), :],
                        sems.at[k, q, j],
                    )
                )
    for c in copies:
        c.start()
    for c in copies:
        c.wait()
    for q, i in enumerate(planes):
        fill_columns(q, i, depth, more_x, f_ref, g_ref, ne, be)
        scale(q, depth, ne, ve)
    for q in (0, 3):
        first_x(q, depth, ve, be, dx)
    for s in range(5):
        for j in range(depth):
            rows = pl.ds(8 * s, 8)
            up_ref[j, rows, :] = ne[3, j, strip(s), :]
            up_ref[j, pl.ds(40 + 8 * s, 8), :] = be[3, j, strip(s), :]
            down_ref[j, rows, :] = ne[0, j, strip(s), :]
    for s in range(4):
        div = cross_divergence(3, s, depth, ve, be, dx)[-1]
        for j in range(depth):
            before = clip(ve[3, j, strip(s), :] - ve[2, j, strip(s), :], be[2, j, strip(s), :])
            up_ref[j, pl.ds(80 + 8 * s, 8), :] = div[j] - before
        div = cross_divergence(0, s, depth, ve, be, dx)[-1]
        for j in range(depth):
            own = clip(ve[1, j, strip(s), :] - ve[0, j, strip(s), :], be[0, j, strip(s), :])
            down_ref[j, pl.ds(40 + 8 * s, 8), :] = div[j] + own


def planes(flags, noisy, bound, from_prev, from_next):
    depth = noisy.shape[2] // LANES
    buffer = pltpu.VMEM((4, depth, ROWS, LANES), F32)
    return pl.pallas_call(
        planes_kernel,
        out_shape=(
            jax.ShapeDtypeStruct((depth, 112, LANES), F32),
            jax.ShapeDtypeStruct((depth, 72, LANES), F32),
        ),
        in_specs=[pl.BlockSpec(memory_space=pltpu.SMEM)]
        + [pl.BlockSpec(memory_space=pl.ANY)] * 2
        + [pl.BlockSpec(memory_space=pltpu.VMEM)] * 2,
        out_specs=[pl.BlockSpec(memory_space=pltpu.VMEM)] * 2,
        scratch_shapes=[buffer] * 4 + [pltpu.SemaphoreType.DMA((2, 4, depth))],
        compiler_params=pltpu.CompilerParams(vmem_limit_bytes=16 << 20),
        name="pack_planes",
    )(flags, noisy, bound, from_prev, from_next)


CHUNK = 8


def main_kernel(
    flags, n_hbm, b_hbm, f_ref, g_ref, up_ref, down_ref,
    u_hbm, d_hbm, sums_ref,
    ne, be, ve, ue, di, dx, dz, dx2, di2, div1, uo, do, in_sems, u_sems, d_sems,
):
    ni, depth = n_hbm.shape[0], n_hbm.shape[2] // LANES
    more_i, more_x = flags[0] > 0, flags[1] > 0
    chunks = ni // CHUNK

    def reads(c):
        return [
            pltpu.make_async_copy(
                src.at[pl.ds(c * CHUNK, CHUNK), :, pl.ds(j * LANES, LANES)],
                dst.at[pl.ds(c * CHUNK + 1, CHUNK), j, pl.ds(OWN, 32), :],
                in_sems.at[k, j, c],
            )
            for k, (src, dst) in enumerate(((n_hbm, ne), (b_hbm, be)))
            for j in range(depth)
        ]

    def writes(c):
        span = pl.ds(c * CHUNK, CHUNK)
        return [pltpu.make_async_copy(uo.at[span], u_hbm.at[span], u_sems.at[c])] + [
            pltpu.make_async_copy(do.at[k, span], d_hbm.at[k, span], d_sems.at[k, c])
            for k in range(3)
        ]

    for c in range(chunks):
        for copy in reads(c):
            copy.start()

    for j in range(depth):
        for s in range(5):
            ne[0, j, strip(s), :] = up_ref[j, pl.ds(8 * s, 8), :]
            be[0, j, strip(s), :] = up_ref[j, pl.ds(40 + 8 * s, 8), :]
    scale(0, depth, ne, ve)

    for copy in reads(0):
        copy.wait()
    fill_columns(1, 0, depth, more_x, f_ref, g_ref, ne, be)
    scale(1, depth, ne, ve)

    for j in range(depth):
        for s in range(5):
            low = clip(ve[1, j, strip(s), :] - ve[0, j, strip(s), :], be[0, j, strip(s), :])
            di[0, j, strip(s), :] = low
            if s < 4:
                part = up_ref[j, pl.ds(80 + 8 * s, 8), :]
                ue[0, j, strip(s), :] = ve[0, j, strip(s), :] + TWO_CS * (part + low)

    def first(p, sums):
        p1, d1 = sums
        first_x(p, depth, ve, be, dx)
        for s in range(5):
            v, b, x, z, div = cross_divergence(p, s, depth, ve, be, dx)
            for j in range(depth):
                i_new = clip(ve[p + 1, j, strip(s), :] - v[j], b[j])
                di[p, j, strip(s), :] = i_new
                total = div[j] + (i_new - di[p - 1, j, strip(s), :])
                ue[p, j, strip(s), :] = v[j] + TWO_CS * total
                if s < 4:
                    dz[p, j, strip(s), :] = z[j]
                    div1[p, j, strip(s), :] = total
                    p1 = p1 + total * total
                    d1 = d1 + (x[j] * x[j] + (i_new * i_new + z[j] * z[j]))
        for j in range(depth):
            edge = ue[p, j, pl.ds(HALO - 1, 1), :]
            ue[p, j, pl.ds(HALO, 1), :] = jnp.where(more_x, ue[p, j, pl.ds(HALO, 1), :], edge)
            ue[p, j, pl.ds(HALO + 8, 1), :] = ue[p, j, pl.ds(OWN, 1), :]
        return p1, d1

    def second_i(p, s, j):
        low = clip(
            di[p, j, strip(s), :] + (ue[p + 1, j, strip(s), :] - ue[p, j, strip(s), :]),
            be[p, j, strip(s), :],
        )
        di2[p, j, strip(s), :] = low
        return low

    def second(p, sums):
        p2, d2 = sums
        i = p - 1
        for j in range(depth):
            for s in (4, 3, 2, 1, 0):
                dx2[p, j, strip(s), :] = clip(
                    dx[p, j, strip(s), :]
                    + (ue[p, j, strip_next(s), :] - ue[p, j, strip(s), :]),
                    be[p, j, strip(s), :],
                )
            dx2[p, j, pl.ds(OWN - 1, 1), :] = dx2[p, j, pl.ds(HALO + 7, 1), :]
        for s in range(4):
            u = [ue[p, j, strip(s), :] for j in range(depth)]
            z_old = [dz[p, j, strip(s), :] for j in range(depth)]
            z_new = [
                clip(o + (n - w), be[p, j, strip(s), :])
                for j, (o, n, w) in enumerate(zip(z_old, depth_next(u), u))
            ]
            back = depth_back(z_new)
            rows = pl.ds(8 * s, 8)
            for j in range(depth):
                lanes = pl.ds(j * LANES, LANES)
                i_new = second_i(p, s, j)
                x_new = dx2[p, j, strip(s), :]
                total = (
                    (x_new - dx2[p, j, strip_back(s), :])
                    + (z_new[j] - back[j])
                    + (i_new - di2[p - 1, j, strip(s), :])
                )
                old = div1[p, j, strip(s), :]
                uo[i, rows, lanes] = ne[p, j, strip(s), :] + (C * total + C_OLD * old)
                do[0, i, rows, lanes] = i_new
                do[1, i, rows, lanes] = x_new
                do[2, i, rows, lanes] = z_new[j]
                gap = total - C * old
                p2 = p2 + gap * gap
                gi = i_new - di[p, j, strip(s), :]
                gx = x_new - dx[p, j, strip(s), :]
                gz = z_new[j] - z_old[j]
                d2 = d2 + (gi * gi + (gx * gx + gz * gz))
        return p2, d2

    zero = jnp.zeros((8, LANES), F32)

    def upper(p):
        @pl.when(p < ni)
        def _():
            @pl.when(p % CHUNK == 0)
            def _():
                for copy in reads(p // CHUNK):
                    copy.wait()

            fill_columns(p + 1, p, depth, more_x, f_ref, g_ref, ne, be)

        @pl.when(p == ni)
        def _():
            for j in range(depth):
                for s in range(5):
                    ne[ni + 1, j, strip(s), :] = jnp.where(
                        more_i, down_ref[j, pl.ds(8 * s, 8), :], ne[ni, j, strip(s), :]
                    )

        scale(p + 1, depth, ne, ve)

    upper(1)
    first_sums = first(1, (zero, zero))
    for s in range(4):
        for j in range(depth):
            second_i(0, s, j)

    def body(p, carry):
        a, b = carry
        upper(p)
        a = first(p, a)
        b = second(p - 1, b)

        @pl.when((p - 1) % CHUNK == 0)
        def _():
            for copy in writes((p - 1) // CHUNK - 1):
                copy.start()

        return a, b

    first_sums, second_sums = lax.fori_loop(
        2, ni + 1, body, (first_sums, (zero, zero))
    )
    for j in range(depth):
        for s in range(4):
            part = down_ref[j, pl.ds(40 + 8 * s, 8), :]
            top = ve[ni + 1, j, strip(s), :] + TWO_CS * (part - di[ni, j, strip(s), :])
            ue[ni + 1, j, strip(s), :] = jnp.where(more_i, top, ue[ni, j, strip(s), :])
    second_sums = second(ni, second_sums)
    for copy in writes(chunks - 1):
        copy.start()
    sums = first_sums + second_sums
    factors = (C * C, 1.0, C * C, 1.0)
    lane = lax.broadcasted_iota(jnp.int32, (1, LANES), 1)
    row = jnp.zeros((1, LANES), F32)
    for k in range(4):
        row = jnp.where(lane == k, factors[k] * jnp.sum(sums[k]), row)
    sums_ref[...] = row
    for c in range(chunks):
        for copy in writes(c):
            copy.wait()


def iterate(flags, noisy, bound, from_prev, from_next, from_below, from_above):
    ni, nx, nz = noisy.shape
    depth = nz // LANES
    buffer = pltpu.VMEM((ni + 2, depth, ROWS, LANES), F32)
    chunks = ni // CHUNK
    return pl.pallas_call(
        main_kernel,
        out_shape=(
            jax.ShapeDtypeStruct((ni, nx, nz), F32),
            jax.ShapeDtypeStruct((3, ni, nx, nz), F32),
            jax.ShapeDtypeStruct((1, LANES), F32),
        ),
        in_specs=[pl.BlockSpec(memory_space=pltpu.SMEM)]
        + [pl.BlockSpec(memory_space=pl.ANY)] * 2
        + [pl.BlockSpec(memory_space=pltpu.VMEM)] * 4,
        out_specs=[pl.BlockSpec(memory_space=pl.ANY)] * 2
        + [pl.BlockSpec(memory_space=pltpu.VMEM)],
        scratch_shapes=[buffer] * 10
        + [
            pltpu.VMEM((ni, nx, nz), F32),
            pltpu.VMEM((3, ni, nx, nz), F32),
            pltpu.SemaphoreType.DMA((2, depth, chunks)),
            pltpu.SemaphoreType.DMA((chunks,)),
            pltpu.SemaphoreType.DMA((3, chunks)),
        ],
        compiler_params=pltpu.CompilerParams(vmem_limit_bytes=58 << 20),
        name="iterate",
    )(flags, noisy, bound, from_prev, from_next, from_below, from_above)


def per_device(noisy, bound):
    count_i, count_x = lax.axis_size("inl"), lax.axis_size("xln")
    flags = jnp.stack(
        [
            (lax.axis_index("inl") < count_i - 1).astype(jnp.int32),
            (lax.axis_index("xln") < count_x - 1).astype(jnp.int32),
        ]
    )
    to_next, to_prev = pack(noisy, bound)
    from_prev = sent_along(to_next, "xln", 1)
    from_next = sent_along(to_prev, "xln", -1)
    up, down = planes(flags, noisy, bound, from_prev, from_next)
    from_below = sent_along(up, "inl", 1)
    from_above = sent_along(down, "inl", -1)
    primal, dual, sums = iterate(
        flags, noisy, bound, from_prev, from_next, from_below, from_above
    )
    devices = count_i * count_x
    spread = jnp.broadcast_to(sums[:, :4], (devices, 4))
    parts = lax.all_to_all(spread, AXES, 0, 0, tiled=True)
    norms = jnp.sqrt(jnp.sum(parts, axis=0)).reshape(2, 2)
    return primal, dual, norms


def solution(mesh):
    in_specs = (P("inl", "xln", None), P("inl", "xln", None))
    out_specs = (P("inl", "xln", None), P(None, "inl", "xln", None), P())
    return jax.shard_map(
        per_device, mesh=mesh, in_specs=in_specs, out_specs=out_specs, check_vma=False
    )
```

```python
import jax
import jax.numpy as jnp
from jax import lax
from jax.experimental import pallas as pl
from jax.experimental.pallas import tpu as pltpu
from jax.sharding import PartitionSpec as P

SIGMA = 0.28
TAU = 0.28
C = TAU / (1.0 + TAU)
C_OLD = C / (1.0 + TAU)
TWO_CS = 2.0 * C * SIGMA

LANES = 128
ROWS = 56
OWN = 8
HALO = 40
AXES = ("inl", "xln")
F32 = jnp.float32


def swapped(value, axis, first):
    count = lax.axis_size(axis)
    pairs = []
    for low in range(first, count - 1, 2):
        pairs += [(low, low + 1), (low + 1, low)]
    return lax.ppermute(value, axis, pairs)


def clip(value, bound):
    return jnp.minimum(jnp.maximum(value, -bound), bound)


def last_lane():
    return lax.broadcasted_iota(jnp.int32, (8, LANES), 1) == LANES - 1


def first_lane():
    return lax.broadcasted_iota(jnp.int32, (8, LANES), 1) == 0


def depth_next(tiles):
    rolled = [pltpu.roll(t, LANES - 1, 1) for t in tiles] + [tiles[-1]]
    mask = last_lane()
    return [jnp.where(mask, rolled[j + 1], rolled[j]) for j in range(len(tiles))]


def depth_back(tiles):
    rolled = [jnp.zeros((8, LANES), F32)] + [pltpu.roll(t, 1, 1) for t in tiles]
    mask = first_lane()
    return [jnp.where(mask, rolled[j], rolled[j + 1]) for j in range(len(tiles))]


def pack_kernel(flags, n_hbm, b_hbm, a_ref, c_ref, n4_ref, b4_ref, slab, sems, plane_sems):
    ni, nx, depth = n_hbm.shape[0], n_hbm.shape[1], n_hbm.shape[2] // LANES
    even = flags[3] == 0
    columns, planes = [], []
    for k, src in enumerate((n_hbm, b_hbm)):
        for m, start in enumerate((jnp.where(even, nx - 8, 0), jnp.where(even, 0, nx - 8))):
            start = pl.multiple_of(start, 8)
            columns.append(
                pltpu.make_async_copy(src.at[:, pl.ds(start, 8), :], slab.at[m, k], sems.at[m, k])
            )
    for k, (src, dst) in enumerate(((n_hbm, n4_ref), (b_hbm, b4_ref))):
        for q, i in enumerate((0, ni - 2)):
            planes.append(
                pltpu.make_async_copy(
                    src.at[pl.ds(i, 2)], dst.at[pl.ds(2 * q, 2)], plane_sems.at[k, q]
                )
            )
    for c in columns + planes:
        c.start()
    for c in columns:
        c.wait()

    def body(i, _):
        for k in range(2):
            for j in range(depth):
                lanes = pl.ds(j * LANES, LANES)
                a_ref[i, j, 2 * k : 2 * k + 2, :] = jnp.where(
                    even, slab[0, k, i, 6:8, lanes], slab[0, k, i, 0:2, lanes]
                )
                c_ref[i, j, 2 * k : 2 * k + 2, :] = jnp.where(
                    even, slab[1, k, i, 0:2, lanes], slab[1, k, i, 6:8, lanes]
                )
        return 0

    lax.fori_loop(0, ni, body, 0, unroll=2)
    for c in planes:
        c.wait()


HBM = pltpu.MemorySpace.HBM
VMEM = pltpu.MemorySpace.VMEM


def pack(flags, noisy, bound):
    ni, nx, nz = noisy.shape
    depth = nz // LANES
    message = pltpu.VMEM((ni, depth, 4, LANES), F32)
    boundary = pltpu.VMEM((4, nx, nz), F32)
    return pl.pallas_call(
        pack_kernel,
        out_shape=(message, message, boundary, boundary),
        in_specs=[pl.BlockSpec(memory_space=pltpu.SMEM)] + [pl.BlockSpec(memory_space=HBM)] * 2,
        out_specs=[pl.BlockSpec(memory_space=VMEM)] * 4,
        scratch_shapes=[
            pltpu.VMEM((2, 2, ni, 8, nz), F32),
            pltpu.SemaphoreType.DMA((2, 2)),
            pltpu.SemaphoreType.DMA((2, 2)),
        ],
        compiler_params=pltpu.CompilerParams(vmem_limit_bytes=8 << 20),
        name="pack_faces",
    )(flags, noisy, bound)


def strip(s):
    return pl.ds(OWN + 8 * s, 8)


def strip_next(s):
    return pl.ds(OWN + 8 * s + 1, 8)


def strip_back(s):
    return pl.ds(OWN + 8 * s - 1, 8)


def wrap_rows(field, p, depth):
    for j in range(depth):
        field[p, j, pl.ds(HALO + 8, 1), :] = field[p, j, pl.ds(OWN, 1), :]


def scale(p, depth, image_of, ve):
    for j in range(depth):
        for s in range(5):
            ve[p, j, strip(s), :] = SIGMA * image_of(p, j, s)
    wrap_rows(ve, p, depth)


def tile(field, p, j, s):
    return field[p, pl.ds(8 * s, 8), pl.ds(j * LANES, LANES)]


def x_dual(p, s, depth, ve, v, b, c):
    return [
        clip2(ve[p, j, strip_next(s), :] - v[j], b[j], c[j]) for j in range(depth)
    ]


def clip2(value, bound, below):
    return jnp.minimum(jnp.maximum(value, below), bound)


ORDER = (4, 0, 1, 2, 3)


def crossline(p, q, depth, ve, bound_of, dx, then):
    for s in (3,) + ORDER:
        v = [ve[p, j, strip(s), :] for j in range(depth)]
        b = [bound_of(p, j, s) for j in range(depth)]
        c = [-k for k in b]
        x = x_dual(p, s, depth, ve, v, b, c)
        for j in range(depth):
            dx[q, j, strip(s), :] = x[j]
        if s == 3:
            break
    for s in ORDER:
        v = [ve[p, j, strip(s), :] for j in range(depth)]
        b = [bound_of(p, j, s) for j in range(depth)]
        c = [-k for k in b]
        if s == 3:
            x = [dx[q, j, strip(s), :] for j in range(depth)]
        else:
            x = x_dual(p, s, depth, ve, v, b, c)
            for j in range(depth):
                dx[q, j, strip(s), :] = x[j]
        z = [clip2(n - o, k, m) for n, o, k, m in zip(depth_next(v), v, b, c)]
        back = depth_back(z)
        div = [x[j] - dx[q, j, strip_back(s), :] + (z[j] - back[j]) for j in range(depth)]
        then(s, v, b, c, x, z, div)
        if s == 4:
            for j in range(depth):
                dx[q, j, pl.ds(OWN - 1, 1), :] = dx[q, j, pl.ds(HALO + 7, 1), :]


def planes_kernel(
    flags, n4_ref, b4_ref, sent_a, sent_c, got_a, got_c,
    a_ref, c_ref, hn, hb, ve, dx,
):
    ni, depth = got_a.shape[0], got_a.shape[1]
    more_x, even_x, even_i = flags[1] > 0, flags[3] == 0, flags[2] == 0

    def sort(i, _):
        for j in range(depth):
            last = jnp.where(even_x, sent_a[i, j, 1:2, :], sent_c[i, j, 1:2, :])
            a_n, c_n = got_a[i, j, 0:2, :], got_c[i, j, 0:2, :]
            a_b, c_b = got_a[i, j, 2:4, :], got_c[i, j, 2:4, :]
            hn[i, j, 6:8, :] = jnp.where(even_x, c_n, a_n)
            hb[i, j, 6:8, :] = jnp.where(even_x, c_b, a_b)
            above = jnp.where(even_x, a_n, c_n)
            hn[i, j, 0:2, :] = above
            hb[i, j, 0:2, :] = jnp.where(even_x, a_b, c_b)
            hn[i, j, 0:1, :] = jnp.where(more_x, above[0:1], last)
        return 0

    lax.fori_loop(0, ni, sort, 0, unroll=2)
    place = (0, 1, ni - 2, ni - 1)

    def image_of(q, j, s):
        return hn[place[q], j, 0:8, :] if s == 4 else tile(n4_ref, q, j, s)

    def bound_of(q, j, s):
        return hb[place[q], j, 0:8, :] if s == 4 else tile(b4_ref, q, j, s)

    for q in range(4):
        scale(q, depth, image_of, ve)

    def up(ref):
        for s in range(5):
            for j in range(depth):
                ref[j, pl.ds(8 * s, 8), :] = image_of(3, j, s)
                ref[j, pl.ds(40 + 8 * s, 8), :] = bound_of(3, j, s)

        def then(s, v, b, c, x, z, div):
            if s == 4:
                return
            for j in range(depth):
                before = clip(v[j] - ve[2, j, strip(s), :], bound_of(2, j, s))
                ref[j, pl.ds(80 + 8 * s, 8), :] = div[j] - before

        crossline(3, 3, depth, ve, bound_of, dx, then)

    def down(ref):
        for s in range(5):
            for j in range(depth):
                ref[j, pl.ds(8 * s, 8), :] = image_of(0, j, s)

        def then(s, v, b, c, x, z, div):
            if s == 4:
                return
            for j in range(depth):
                own = clip2(ve[1, j, strip(s), :] - v[j], b[j], c[j])
                ref[j, pl.ds(40 + 8 * s, 8), :] = div[j] + own

        crossline(0, 0, depth, ve, bound_of, dx, then)

    @pl.when(even_i)
    def _():
        up(a_ref)
        down(c_ref)

    @pl.when(jnp.logical_not(even_i))
    def _():
        down(a_ref)
        up(c_ref)


def planes(flags, n4, b4, sent_a, sent_c, got_a, got_c):
    ni, depth = got_a.shape[0], got_a.shape[1]
    buffer = pltpu.VMEM((4, depth, ROWS, LANES), F32)
    return pl.pallas_call(
        planes_kernel,
        out_shape=(pltpu.VMEM((depth, 112, LANES), F32),) * 2
        + (pltpu.VMEM((ni, depth, 8, LANES), F32),) * 2,
        in_specs=[pl.BlockSpec(memory_space=pltpu.SMEM)] + [pl.BlockSpec(memory_space=VMEM)] * 6,
        out_specs=[pl.BlockSpec(memory_space=VMEM)] * 4,
        scratch_shapes=[buffer] * 2,
        compiler_params=pltpu.CompilerParams(vmem_limit_bytes=8 << 20),
        name="pack_planes",
    )(flags, n4, b4, sent_a, sent_c, got_a, got_c)


class Fields:
    def __init__(self, ring, **fields):
        self.ring = ring
        self.__dict__.update(fields)


class Split:
    def __init__(self, given, own, slots):
        self.given, self.own, self.slots = given, own, slots

    def __getitem__(self, index):
        return (self.given if index[0] in self.slots else self.own)[index]

    def __setitem__(self, index, value):
        self.own[index] = value


def first(t, p, depth, more_x, sums):
    sums = list(sums)
    q, before = t.ring(p), t.ring(p - 1)

    def then(s, v, b, c, x, z, div):
        for j in range(depth):
            i_new = clip2(t.ve[p + 1, j, strip(s), :] - v[j], b[j], c[j])
            t.di[q, j, strip(s), :] = i_new
            total = div[j] + (i_new - t.di[before, j, strip(s), :])
            t.ue[p, j, strip(s), :] = v[j] + TWO_CS * total
            if s < 4:
                t.dz[q, j, strip(s), :] = z[j]
                t.div1[q, j, strip(s), :] = total
                sums[0] = sums[0] + total * total
                sums[1] = sums[1] + (x[j] * x[j] + (i_new * i_new + z[j] * z[j]))

    crossline(p, q, depth, t.ve, t.bound_of, t.dx, then)
    for j in range(depth):
        edge = t.ue[p, j, pl.ds(HALO - 1, 1), :]
        t.ue[p, j, pl.ds(HALO, 1), :] = jnp.where(more_x, t.ue[p, j, pl.ds(HALO, 1), :], edge)
    wrap_rows(t.ue, p, depth)
    return tuple(sums)


def second_i(t, p, s, j):
    q = t.ring(p)
    t.di2[q, j, strip(s), :] = clip(
        t.di[q, j, strip(s), :] + (t.ue[p + 1, j, strip(s), :] - t.ue[p, j, strip(s), :]),
        t.bound_of(p, j, s),
    )


def second(t, p, o, depth, sums, uo, do):
    p2, d2 = sums
    q, before = t.ring(p), t.ring(p - 1)
    for s in ORDER:
        u = [t.ue[p, j, strip(s), :] for j in range(depth)]
        b = [t.bound_of(p, j, s) for j in range(depth)]
        c = [-k for k in b]
        x_old = [t.dx[q, j, strip(s), :] for j in range(depth)]
        x_new = [
            clip2(x_old[j] + (t.ue[p, j, strip_next(s), :] - u[j]), b[j], c[j])
            for j in range(depth)
        ]
        for j in range(depth):
            t.dx2[q, j, strip(s), :] = x_new[j]
        if s == 4:
            for j in range(depth):
                t.dx2[q, j, pl.ds(OWN - 1, 1), :] = t.dx2[q, j, pl.ds(HALO + 7, 1), :]
            continue
        z_old = [t.dz[q, j, strip(s), :] for j in range(depth)]
        z_new = [
            clip2(z_old[j] + (n - u[j]), b[j], c[j]) for j, n in enumerate(depth_next(u))
        ]
        back = depth_back(z_new)
        rows = pl.ds(8 * s, 8)
        for j in range(depth):
            lanes = pl.ds(j * LANES, LANES)
            i_old = t.di[q, j, strip(s), :]
            i_new = clip2(i_old + (t.ue[p + 1, j, strip(s), :] - u[j]), b[j], c[j])
            t.di2[q, j, strip(s), :] = i_new
            total = (
                (x_new[j] - t.dx2[q, j, strip_back(s), :])
                + (z_new[j] - back[j])
                + (i_new - t.di2[before, j, strip(s), :])
            )
            old = t.div1[q, j, strip(s), :]
            uo[o, rows, lanes] = t.image_of(p, j, s) + (C * total + C_OLD * old)
            do[0, o, rows, lanes] = i_new
            do[1, o, rows, lanes] = x_new[j]
            do[2, o, rows, lanes] = z_new[j]
            gap = total - C * old
            p2 = p2 + gap * gap
            gi = i_new - i_old
            gx = x_new[j] - x_old[j]
            gz = z_new[j] - z_old[j]
            d2 = d2 + (gi * gi + (gx * gx + gz * gz))
    return p2, d2


KEPT = {1: 0, 2: 1, 5: 2, 6: 3}


def boundary_planes(ni):
    return 0, 1, ni - 2, ni - 1


CHUNK = 4
PART = 2
HANDED = (
    ("ve", (1, 2, 5, 6)),
    ("ue", (2, 3, 4, 5)),
    ("di", (2, 5)),
    ("dx", (2, 5)),
    ("dz", (2, 5)),
    ("div1", (2, 5)),
    ("di2", (4,)),
)


def inner_kernel(flags, n_hbm, b_hbm, hn, hb, u_hbm, d_hbm, sums_ref, *refs):
    handed, refs = refs[: len(HANDED)], refs[len(HANDED) :]
    ne, be, ve, ue, di, dx, dz, div1, dx2, di2, uo, do, in_sems, u_sems, d_sems = refs
    ni, depth = n_hbm.shape[0], n_hbm.shape[2] // LANES
    more_x = flags[1] > 0

    def bound_of(p, j, s):
        return hb[p, j, 0:8, :] if s == 4 else tile(be, p, j, s)

    def image_of(p, j, s):
        return hn[p, j, 0:8, :] if s == 4 else tile(ne, p, j, s)

    t = Fields(
        lambda p: p % 4,
        bound_of=bound_of, image_of=image_of, ve=ve, ue=ue, di=di, dx=dx, dz=dz, div1=div1, dx2=dx2, di2=di2,
    )
    chunks, parts = ni // CHUNK, (ni - 4) // PART

    def reads(c):
        span = pl.ds(c * CHUNK, CHUNK)
        return [
            pltpu.make_async_copy(src.at[span], dst.at[span], in_sems.at[k, c])
            for k, (src, dst) in enumerate(((n_hbm, ne), (b_hbm, be)))
        ]

    def writes(c):
        span = pl.ds(c * PART + 2, PART)
        return [pltpu.make_async_copy(uo.at[span], u_hbm.at[span], u_sems.at[c])] + [
            pltpu.make_async_copy(do.at[k, span], d_hbm.at[k, span], d_sems.at[k, c])
            for k in range(3)
        ]

    def hand(slots):
        for ref, (name, wanted) in zip(handed, HANDED):
            field = getattr(t, name)
            short = name in ("di", "dx", "dz", "div1", "di2")
            for slot in wanted:
                if slot in slots:
                    plane = slot - 1 if slot < 4 else ni - 7 + slot
                    place = plane % 4 if short else plane
                    for j in range(depth):
                        for s in range(5):
                            if s < 4 or name not in ("dz", "div1", "di2"):
                                ref[slot, j, strip(s), :] = field[place, j, strip(s), :]
                        if name in ("ve", "ue"):
                            ref[slot, j, pl.ds(HALO + 8, 1), :] = field[place, j, pl.ds(HALO + 8, 1), :]

    def ready(p):
        scale(p, depth, image_of, ve)

    for c in range(chunks):
        for copy in reads(c):
            copy.start()
    for copy in reads(0):
        copy.wait()
    for p in range(4):
        ready(p)
    for j in range(depth):
        for s in range(5):
            di[0, j, strip(s), :] = clip(
                ve[1, j, strip(s), :] - ve[0, j, strip(s), :], bound_of(0, j, s)
            )
    zero = jnp.zeros((8, LANES), F32)
    a = first(t, 1, depth, more_x, (zero, zero))
    a = first(t, 2, depth, more_x, a)
    for s in range(4):
        for j in range(depth):
            second_i(t, 1, s, j)
    hand((1, 2, 3))

    def body(p, carry):
        a, b = carry

        @pl.when((p + 1) % CHUNK == 0)
        def _():
            for copy in reads((p + 1) // CHUNK):
                copy.wait()

        ready(p + 1)
        a = first(t, p, depth, more_x, a)
        b = second(t, p - 1, p - 1, depth, b, uo, do)

        @pl.when(p % PART == 0)
        def _():
            for copy in writes(p // PART - 2):
                copy.start()

        return a, b

    a, b = lax.fori_loop(3, ni - 1, body, (a, (zero, zero)))
    hand((4, 5, 6))
    for k, total in enumerate(a + b):
        sums_ref[k] = total
    for c in range(parts):
        for copy in writes(c):
            copy.wait()


def inner(flags, noisy, bound, halo_n, halo_b):
    ni, nx, nz = noisy.shape
    depth = nz // LANES
    full = pltpu.VMEM((ni, depth, ROWS, LANES), F32)
    short = pltpu.VMEM((4, depth, ROWS, LANES), F32)
    chunks, parts = ni // CHUNK, (ni - 4) // PART
    slots = jax.ShapeDtypeStruct((8, depth, ROWS, LANES), F32)
    return pl.pallas_call(
        inner_kernel,
        out_shape=(
            jax.ShapeDtypeStruct((ni, nx, nz), F32),
            jax.ShapeDtypeStruct((3, ni, nx, nz), F32),
            jax.ShapeDtypeStruct((4, 8, LANES), F32),
        )
        + (slots,) * len(HANDED),
        in_specs=[pl.BlockSpec(memory_space=pltpu.SMEM)]
        + [pl.BlockSpec(memory_space=HBM)] * 2
        + [pl.BlockSpec(memory_space=VMEM)] * 2,
        out_specs=[pl.BlockSpec(memory_space=HBM)] * 2
        + [pl.BlockSpec(memory_space=VMEM)] * (1 + len(HANDED)),
        scratch_shapes=[pltpu.VMEM((ni, nx, nz), F32)] * 2
        + [full] * 2
        + [short] * 6
        + [
            pltpu.VMEM((ni, nx, nz), F32),
            pltpu.VMEM((3, ni, nx, nz), F32),
            pltpu.SemaphoreType.DMA((2, chunks)),
            pltpu.SemaphoreType.DMA((parts,)),
            pltpu.SemaphoreType.DMA((3, parts)),
        ],
        compiler_params=pltpu.CompilerParams(vmem_limit_bytes=42 << 20),
        cost_estimate=pl.CostEstimate(flops=200_000_000, transcendentals=0, bytes_accessed=12 << 20),
        name="inner_planes",
    )(flags, noisy, bound, halo_n, halo_b)


def edge_kernel(flags, got_a, got_c, n4_ref, b4_ref, hb, sums_ref, *refs):
    given = dict(zip([name for name, _ in HANDED], refs))
    refs = refs[len(HANDED) :]
    _, _, u_hbm, d_hbm, spread_ref = refs[:5]
    ve, ue, di, dx, dz, div1, di2, dx2, uo, do, u_sems, d_sems = refs[5:]
    own = dict(ve=ve, ue=ue, di=di, dx=dx, dz=dz, div1=div1, di2=di2)
    depth, ni = got_a.shape[0], u_hbm.shape[0]
    more_i, more_x, even_i = flags[0] > 0, flags[1] > 0, flags[2] == 0

    def up(j, row):
        rows = pl.ds(row, 8)
        return jnp.where(even_i, got_c[j, rows, :], got_a[j, rows, :])

    def down(j, row):
        rows = pl.ds(row, 8)
        return jnp.where(even_i, got_a[j, rows, :], got_c[j, rows, :])

    def bound_of(p, j, s):
        if p == 0:
            return up(j, 40 + 8 * s)
        return hb[boundary_planes(ni)[KEPT[p]], j, 0:8, :] if s == 4 else tile(b4_ref, KEPT[p], j, s)

    t = Fields(
        lambda p: p,
        dx2=dx2,
        bound_of=bound_of,
        image_of=lambda p, j, s: tile(n4_ref, KEPT[p], j, s),
        **{name: Split(given[name], own[name], slots) for name, slots in HANDED},
    )
    a = sums_ref[0], sums_ref[1]
    b = sums_ref[2], sums_ref[3]

    for j in range(depth):
        for s in range(5):
            t.ve[0, j, strip(s), :] = SIGMA * up(j, 8 * s)
            t.ve[7, j, strip(s), :] = jnp.where(
                more_i, SIGMA * down(j, 8 * s), t.ve[6, j, strip(s), :]
            )
    for j in range(depth):
        for s in range(5):
            low = clip(t.ve[1, j, strip(s), :] - t.ve[0, j, strip(s), :], up(j, 40 + 8 * s))
            t.di[0, j, strip(s), :] = low
            if s < 4:
                part = up(j, 80 + 8 * s)
                t.ue[0, j, strip(s), :] = t.ve[0, j, strip(s), :] + TWO_CS * (part + low)
    a = first(t, 1, depth, more_x, a)
    for s in range(4):
        for j in range(depth):
            second_i(t, 0, s, j)
    b = second(t, 1, 0, depth, b, uo, do)
    b = second(t, 2, 1, depth, b, uo, do)

    def writes(k, plane):
        at, to = pl.ds(2 * k, 2), pl.ds(plane, 2)
        return [pltpu.make_async_copy(uo.at[at], u_hbm.at[to], u_sems.at[k])] + [
            pltpu.make_async_copy(do.at[c, at], d_hbm.at[c, to], d_sems.at[c, k]) for c in range(3)
        ]

    copies = writes(0, 0)
    for copy in copies:
        copy.start()
    a = first(t, 6, depth, more_x, a)
    for j in range(depth):
        for s in range(4):
            part = down(j, 40 + 8 * s)
            top = t.ve[7, j, strip(s), :] + TWO_CS * (part - t.di[6, j, strip(s), :])
            t.ue[7, j, strip(s), :] = jnp.where(more_i, top, t.ue[6, j, strip(s), :])
    b = second(t, 5, 2, depth, b, uo, do)
    b = second(t, 6, 3, depth, b, uo, do)
    last = writes(1, ni - 2)
    for copy in last:
        copy.start()
    factors = (C * C, 1.0, C * C, 1.0)
    lane = lax.broadcasted_iota(jnp.int32, (1, 4), 1)
    row = jnp.zeros((1, 4), F32)
    for k, total in enumerate(a + b):
        row = jnp.where(lane == k, factors[k] * jnp.sum(total), row)
    spread_ref[...] = jnp.broadcast_to(row, spread_ref.shape)
    for copy in copies + last:
        copy.wait()


def edges(flags, got_a, got_c, n4, b4, halo_b, sums, handed, primal, dual, devices):
    _, nx, nz = primal.shape
    depth = nz // LANES
    buffer = pltpu.VMEM((8, depth, ROWS, LANES), F32)
    count = 7 + len(handed)
    return pl.pallas_call(
        edge_kernel,
        out_shape=(
            jax.ShapeDtypeStruct(primal.shape, F32),
            jax.ShapeDtypeStruct(dual.shape, F32),
            jax.ShapeDtypeStruct((devices, 4), F32),
        ),
        in_specs=[pl.BlockSpec(memory_space=pltpu.SMEM)]
        + [pl.BlockSpec(memory_space=VMEM)] * (count - 1)
        + [pl.BlockSpec(memory_space=HBM)] * 2,
        out_specs=[pl.BlockSpec(memory_space=HBM)] * 2 + [pl.BlockSpec(memory_space=VMEM)],
        scratch_shapes=[buffer] * 8
        + [
            pltpu.VMEM((4, nx, nz), F32),
            pltpu.VMEM((3, 4, nx, nz), F32),
            pltpu.SemaphoreType.DMA((2,)),
            pltpu.SemaphoreType.DMA((3, 2)),
        ],
        input_output_aliases={count: 0, count + 1: 1},
        compiler_params=pltpu.CompilerParams(vmem_limit_bytes=24 << 20),
        name="edge_planes",
    )(flags, got_a, got_c, n4, b4, halo_b, sums, *handed, primal, dual)


def per_device(noisy, bound):
    count_i, count_x = lax.axis_size("inl"), lax.axis_size("xln")
    at_i, at_x = lax.axis_index("inl"), lax.axis_index("xln")
    flags = jnp.stack(
        [
            (at_i < count_i - 1).astype(jnp.int32),
            (at_x < count_x - 1).astype(jnp.int32),
            at_i % 2,
            at_x % 2,
        ]
    )
    noisy, bound = (pltpu.with_memory_space_constraint(x, HBM) for x in (noisy, bound))
    send_a, send_c, n4, b4 = pack(flags, noisy, bound)
    got_c = swapped(send_c, "xln", 1)
    got_a = swapped(send_a, "xln", 0)
    face_a, face_c, halo_n, halo_b = planes(flags, n4, b4, send_a, send_c, got_a, got_c)
    back_a = swapped(face_a, "inl", 0)
    back_c = swapped(face_c, "inl", 1)
    primal, dual, sums, *handed = inner(flags, noisy, bound, halo_n, halo_b)
    primal, dual, spread = edges(
        flags, back_a, back_c, n4, b4, halo_b, sums, handed, primal, dual, count_i * count_x
    )
    parts = lax.all_to_all(spread, AXES, 0, 0, tiled=True)
    norms = jnp.sqrt(jnp.sum(parts, axis=0)).reshape(2, 2)
    return primal, dual, norms


def solution(mesh):
    in_specs = (P("inl", "xln", None), P("inl", "xln", None))
    out_specs = (P("inl", "xln", None), P(None, "inl", "xln", None), P())
    return jax.shard_map(
        per_device, mesh=mesh, in_specs=in_specs, out_specs=out_specs, check_vma=False
    )
```

```python
import jax
import jax.numpy as jnp
from jax import lax
from jax.experimental import pallas as pl
from jax.experimental.pallas import tpu as pltpu
from jax.sharding import PartitionSpec as P

SIGMA = 0.28
TAU = 0.28
C = TAU / (1.0 + TAU)
C_OLD = C / (1.0 + TAU)
TWO_CS = 2.0 * C * SIGMA

LANES = 128
ROWS = 56
OWN = 8
HALO = 40
AXES = ("inl", "xln")
F32 = jnp.float32


def swapped(value, axis, first):
    count = lax.axis_size(axis)
    pairs = []
    for low in range(first, count - 1, 2):
        pairs += [(low, low + 1), (low + 1, low)]
    return lax.ppermute(value, axis, pairs)


def clip(value, bound):
    return jnp.minimum(jnp.maximum(value, -bound), bound)


def last_lane():
    return lax.broadcasted_iota(jnp.int32, (8, LANES), 1) == LANES - 1


def first_lane():
    return lax.broadcasted_iota(jnp.int32, (8, LANES), 1) == 0


def depth_next(tiles):
    rolled = [pltpu.roll(t, LANES - 1, 1) for t in tiles] + [tiles[-1]]
    mask = last_lane()
    return [jnp.where(mask, rolled[j + 1], rolled[j]) for j in range(len(tiles))]


def depth_back(tiles):
    rolled = [jnp.zeros((8, LANES), F32)] + [pltpu.roll(t, 1, 1) for t in tiles]
    mask = first_lane()
    return [jnp.where(mask, rolled[j], rolled[j + 1]) for j in range(len(tiles))]


def pack_kernel(flags, n_hbm, b_hbm, a_ref, c_ref, n4_ref, b4_ref, slab, sems, plane_sems):
    ni, nx, depth = n_hbm.shape[0], n_hbm.shape[1], n_hbm.shape[2] // LANES
    even = flags[3] == 0
    columns, planes = [], []
    for k, src in enumerate((n_hbm, b_hbm)):
        for m, start in enumerate((nx - 2, 0)):
            columns.append(
                pltpu.make_async_copy(src.at[:, pl.ds(start, 2), :], slab.at[m, k], sems.at[m, k])
            )
    for k, (src, dst) in enumerate(((n_hbm, n4_ref), (b_hbm, b4_ref))):
        for q, i in enumerate((0, ni - 2)):
            planes.append(
                pltpu.make_async_copy(
                    src.at[pl.ds(i, 2)], dst.at[pl.ds(2 * q, 2)], plane_sems.at[k, q]
                )
            )
    for c in columns + planes:
        c.start()
    for c in columns:
        c.wait()

    def body(i, _):
        for k in range(2):
            for j in range(depth):
                lanes = pl.ds(j * LANES, LANES)
                high, low = slab[0, k, i, 0:2, lanes], slab[1, k, i, 0:2, lanes]
                a_ref[i, j, 2 * k : 2 * k + 2, :] = jnp.where(even, high, low)
                c_ref[i, j, 2 * k : 2 * k + 2, :] = jnp.where(even, low, high)
        return 0

    lax.fori_loop(0, ni, body, 0, unroll=2)
    for c in planes:
        c.wait()


HBM = pltpu.MemorySpace.HBM
VMEM = pltpu.MemorySpace.VMEM


def pack(flags, noisy, bound):
    ni, nx, nz = noisy.shape
    depth = nz // LANES
    message = pltpu.VMEM((ni, depth, 4, LANES), F32)
    boundary = pltpu.VMEM((4, nx, nz), F32)
    return pl.pallas_call(
        pack_kernel,
        out_shape=(message, message, boundary, boundary),
        in_specs=[pl.BlockSpec(memory_space=pltpu.SMEM)] + [pl.BlockSpec(memory_space=HBM)] * 2,
        out_specs=[pl.BlockSpec(memory_space=VMEM)] * 4,
        scratch_shapes=[
            pltpu.VMEM((2, 2, ni, 2, nz), F32),
            pltpu.SemaphoreType.DMA((2, 2)),
            pltpu.SemaphoreType.DMA((2, 2)),
        ],
        compiler_params=pltpu.CompilerParams(vmem_limit_bytes=8 << 20),
        name="pack_faces",
    )(flags, noisy, bound)


def strip(s):
    return pl.ds(OWN + 8 * s, 8)


def strip_next(s):
    return pl.ds(OWN + 8 * s + 1, 8)


def strip_back(s):
    return pl.ds(OWN + 8 * s - 1, 8)


def wrap_rows(field, p, depth):
    for j in range(depth):
        field[p, j, pl.ds(HALO + 8, 1), :] = field[p, j, pl.ds(OWN, 1), :]


def scale(p, depth, image_of, ve):
    for j in range(depth):
        for s in range(5):
            ve[p, j, strip(s), :] = SIGMA * image_of(p, j, s)
    wrap_rows(ve, p, depth)


def tile(field, p, j, s):
    return field[p, pl.ds(8 * s, 8), pl.ds(j * LANES, LANES)]


def x_dual(p, s, depth, ve, v, b, c):
    return [
        clip2(ve[p, j, strip_next(s), :] - v[j], b[j], c[j]) for j in range(depth)
    ]


def clip2(value, bound, below):
    return jnp.minimum(jnp.maximum(value, below), bound)


ORDER = (4, 0, 1, 2, 3)


def crossline(p, q, depth, ve, bound_of, dx, then):
    for s in (3,) + ORDER:
        v = [ve[p, j, strip(s), :] for j in range(depth)]
        b = [bound_of(p, j, s) for j in range(depth)]
        c = [-k for k in b]
        x = x_dual(p, s, depth, ve, v, b, c)
        for j in range(depth):
            dx[q, j, strip(s), :] = x[j]
        if s == 3:
            break
    for s in ORDER:
        v = [ve[p, j, strip(s), :] for j in range(depth)]
        b = [bound_of(p, j, s) for j in range(depth)]
        c = [-k for k in b]
        if s == 3:
            x = [dx[q, j, strip(s), :] for j in range(depth)]
        else:
            x = x_dual(p, s, depth, ve, v, b, c)
            for j in range(depth):
                dx[q, j, strip(s), :] = x[j]
        z = [clip2(n - o, k, m) for n, o, k, m in zip(depth_next(v), v, b, c)]
        back = depth_back(z)
        div = [x[j] - dx[q, j, strip_back(s), :] + (z[j] - back[j]) for j in range(depth)]
        then(s, v, b, c, x, z, div)
        if s == 4:
            for j in range(depth):
                dx[q, j, pl.ds(OWN - 1, 1), :] = dx[q, j, pl.ds(HALO + 7, 1), :]


def planes_kernel(
    flags, n4_ref, b4_ref, sent_a, sent_c, got_a, got_c, _,
    a_ref, c_ref, hn, hb, ve, dx,
):
    ni, depth = got_a.shape[0], got_a.shape[1]
    more_x, even_x, even_i = flags[1] > 0, flags[3] == 0, flags[2] == 0

    def sort(i, _):
        for j in range(depth):
            last = jnp.where(even_x, sent_a[i, j, 1:2, :], sent_c[i, j, 1:2, :])
            a_n, c_n = got_a[i, j, 0:2, :], got_c[i, j, 0:2, :]
            a_b, c_b = got_a[i, j, 2:4, :], got_c[i, j, 2:4, :]
            hn[i, j, 6:8, :] = jnp.where(even_x, c_n, a_n)
            hb[i, j, 6:8, :] = jnp.where(even_x, c_b, a_b)
            above = jnp.where(even_x, a_n, c_n)
            hn[i, j, 0:2, :] = above
            hb[i, j, 0:2, :] = jnp.where(even_x, a_b, c_b)
            hn[i, j, 0:1, :] = jnp.where(more_x, above[0:1], last)
        return 0

    lax.fori_loop(0, ni, sort, 0, unroll=2)
    place = (0, 1, ni - 2, ni - 1)

    def image_of(q, j, s):
        return hn[place[q], j, 0:8, :] if s == 4 else tile(n4_ref, q, j, s)

    def bound_of(q, j, s):
        return hb[place[q], j, 0:8, :] if s == 4 else tile(b4_ref, q, j, s)

    for q in range(4):
        scale(q, depth, image_of, ve)

    def up(ref):
        for s in range(5):
            for j in range(depth):
                ref[j, pl.ds(8 * s, 8), :] = image_of(3, j, s)
                ref[j, pl.ds(40 + 8 * s, 8), :] = bound_of(3, j, s)

        def then(s, v, b, c, x, z, div):
            if s == 4:
                return
            for j in range(depth):
                before = clip(v[j] - ve[2, j, strip(s), :], bound_of(2, j, s))
                ref[j, pl.ds(80 + 8 * s, 8), :] = div[j] - before

        crossline(3, 3, depth, ve, bound_of, dx, then)

    def down(ref):
        for s in range(5):
            for j in range(depth):
                ref[j, pl.ds(8 * s, 8), :] = image_of(0, j, s)

        def then(s, v, b, c, x, z, div):
            if s == 4:
                return
            for j in range(depth):
                own = clip2(ve[1, j, strip(s), :] - v[j], b[j], c[j])
                ref[j, pl.ds(40 + 8 * s, 8), :] = div[j] + own

        crossline(0, 0, depth, ve, bound_of, dx, then)

    @pl.when(even_i)
    def _():
        up(a_ref)
        down(c_ref)

    @pl.when(jnp.logical_not(even_i))
    def _():
        down(a_ref)
        up(c_ref)


def planes(flags, n4, b4, sent_a, sent_c, got_a, got_c, after):
    ni, depth = got_a.shape[0], got_a.shape[1]
    buffer = pltpu.VMEM((4, depth, ROWS, LANES), F32)
    return pl.pallas_call(
        planes_kernel,
        out_shape=(pltpu.VMEM((depth, 112, LANES), F32),) * 2
        + (pltpu.VMEM((ni, depth, 8, LANES), F32),) * 2,
        in_specs=[pl.BlockSpec(memory_space=pltpu.SMEM)] + [pl.BlockSpec(memory_space=VMEM)] * 7,
        out_specs=[pl.BlockSpec(memory_space=VMEM)] * 4,
        scratch_shapes=[buffer] * 2,
        compiler_params=pltpu.CompilerParams(vmem_limit_bytes=8 << 20),
        name="pack_planes",
    )(flags, n4, b4, sent_a, sent_c, got_a, got_c, after)


class Fields:
    def __init__(self, ring, **fields):
        self.ring = ring
        self.__dict__.update(fields)


class Split:
    def __init__(self, given, own, slots):
        self.given, self.own, self.slots = given, own, slots

    def __getitem__(self, index):
        return (self.given if index[0] in self.slots else self.own)[index]

    def __setitem__(self, index, value):
        self.own[index] = value


def first(t, p, depth, more_x, sums):
    sums = list(sums)
    q, before = t.ring(p), t.ring(p - 1)

    def then(s, v, b, c, x, z, div):
        for j in range(depth):
            i_new = clip2(t.ve[p + 1, j, strip(s), :] - v[j], b[j], c[j])
            t.di[q, j, strip(s), :] = i_new
            total = div[j] + (i_new - t.di[before, j, strip(s), :])
            t.ue[p, j, strip(s), :] = v[j] + TWO_CS * total
            if s < 4:
                t.dz[q, j, strip(s), :] = z[j]
                t.div1[q, j, strip(s), :] = total
                sums[0] = sums[0] + total * total
                sums[1] = sums[1] + (x[j] * x[j] + (i_new * i_new + z[j] * z[j]))

    crossline(p, q, depth, t.ve, t.bound_of, t.dx, then)
    for j in range(depth):
        edge = t.ue[p, j, pl.ds(HALO - 1, 1), :]
        t.ue[p, j, pl.ds(HALO, 1), :] = jnp.where(more_x, t.ue[p, j, pl.ds(HALO, 1), :], edge)
    wrap_rows(t.ue, p, depth)
    return tuple(sums)


def second_i(t, p, s, j):
    q = t.ring(p)
    t.di2[q, j, strip(s), :] = clip(
        t.di_of(p, j, s) + (t.ue[p + 1, j, strip(s), :] - t.ue[p, j, strip(s), :]),
        t.bound_of(p, j, s),
    )


def second(t, p, o, depth, sums, uo, do):
    p2, d2 = sums
    q, before = t.ring(p), t.ring(p - 1)
    for s in ORDER:
        u = [t.ue[p, j, strip(s), :] for j in range(depth)]
        b = [t.bound_of(p, j, s) for j in range(depth)]
        c = [-k for k in b]
        x_old = [t.dx[q, j, strip(s), :] for j in range(depth)]
        x_new = [
            clip2(x_old[j] + (t.ue[p, j, strip_next(s), :] - u[j]), b[j], c[j])
            for j in range(depth)
        ]
        for j in range(depth):
            t.dx2[q, j, strip(s), :] = x_new[j]
        if s == 4:
            for j in range(depth):
                t.dx2[q, j, pl.ds(OWN - 1, 1), :] = t.dx2[q, j, pl.ds(HALO + 7, 1), :]
            continue
        z_old = [t.dz_of(p, j, s) for j in range(depth)]
        z_new = [
            clip2(z_old[j] + (n - u[j]), b[j], c[j]) for j, n in enumerate(depth_next(u))
        ]
        back = depth_back(z_new)
        rows = pl.ds(8 * s, 8)
        for j in range(depth):
            lanes = pl.ds(j * LANES, LANES)
            i_old = t.di_of(p, j, s)
            i_new = clip2(i_old + (t.ue[p + 1, j, strip(s), :] - u[j]), b[j], c[j])
            t.di2[q, j, strip(s), :] = i_new
            total = (
                (x_new[j] - t.dx2[q, j, strip_back(s), :])
                + (z_new[j] - back[j])
                + (i_new - t.di2[before, j, strip(s), :])
            )
            old = t.div1[q, j, strip(s), :]
            uo[o, rows, lanes] = t.image_of(p, j, s) + (C * total + C_OLD * old)
            do[0, o, rows, lanes] = i_new
            do[1, o, rows, lanes] = x_new[j]
            do[2, o, rows, lanes] = z_new[j]
            gap = total - C * old
            p2 = p2 + gap * gap
            gi = i_new - i_old
            gx = x_new[j] - x_old[j]
            gz = z_new[j] - z_old[j]
            d2 = d2 + (gi * gi + (gx * gx + gz * gz))
    return p2, d2


KEPT = {1: 0, 2: 1, 5: 2, 6: 3}


def boundary_planes(ni):
    return 0, 1, ni - 2, ni - 1


CHUNK = 4
PART = 2
HANDED = (
    ("ve", (1, 2, 5, 6)),
    ("ue", (2, 3, 4, 5)),
    ("di", (2, 5)),
    ("dx", (2, 5)),
    ("dz", (2, 5)),
    ("div1", (2, 5)),
    ("di2", (4,)),
)


def own_kernel(n_hbm, b_hbm, nv, bv, di, dz, part, sum_ref, sems):
    ni, depth = n_hbm.shape[0], n_hbm.shape[2] // LANES
    chunks = ni // CHUNK

    def reads(c):
        span = pl.ds(c * CHUNK, CHUNK)
        return [
            pltpu.make_async_copy(src.at[span], dst.at[span], sems.at[k, c])
            for k, (src, dst) in enumerate(((n_hbm, nv), (b_hbm, bv)))
        ]

    for c in range(chunks):
        for copy in reads(c):
            copy.start()
    for copy in reads(0):
        copy.wait()

    def spot(j, s):
        return pl.ds(8 * s, 8), pl.ds(j * LANES, LANES)

    for s in range(4):
        for j in range(depth):
            gap = SIGMA * (tile(nv, 1, j, s) - tile(nv, 0, j, s))
            di[(0,) + spot(j, s)] = clip(gap, tile(bv, 0, j, s))

    def body(p, total):
        @pl.when((p + 1) % CHUNK == 0)
        def _():
            for copy in reads((p + 1) // CHUNK):
                copy.wait()

        for s in range(4):
            n = [tile(nv, p, j, s) for j in range(depth)]
            b = [tile(bv, p, j, s) for j in range(depth)]
            c = [-k for k in b]
            z = [clip2(SIGMA * (m - o), k, l) for m, o, k, l in zip(depth_next(n), n, b, c)]
            back = depth_back(z)
            for j in range(depth):
                new = clip2(SIGMA * (tile(nv, p + 1, j, s) - n[j]), b[j], c[j])
                at = (p,) + spot(j, s)
                di[at] = new
                dz[at] = z[j]
                part[at] = (new - tile(di, p - 1, j, s)) + (z[j] - back[j])
                total = total + (new * new + z[j] * z[j])
        return total

    sum_ref[...] = lax.fori_loop(1, ni - 1, body, jnp.zeros((8, LANES), F32))


def own(noisy, bound):
    ni, nx, nz = noisy.shape
    whole = pltpu.VMEM((ni, nx, nz), F32)
    return pl.pallas_call(
        own_kernel,
        out_shape=(whole,) * 5 + (pltpu.VMEM((8, LANES), F32),),
        in_specs=[pl.BlockSpec(memory_space=HBM)] * 2,
        out_specs=[pl.BlockSpec(memory_space=VMEM)] * 6,
        scratch_shapes=[pltpu.SemaphoreType.DMA((2, ni // CHUNK))],
        compiler_params=pltpu.CompilerParams(vmem_limit_bytes=16 << 20),
        cost_estimate=pl.CostEstimate(flops=100_000_000, transcendentals=0, bytes_accessed=4 << 20),
        name="own_planes",
    )(noisy, bound)


def inner_kernel(flags, nv, bv, di, dz, part, own_sum, hn, hb, u_hbm, d_hbm, sums_ref, *refs):
    handed, refs = refs[: len(HANDED)], refs[len(HANDED) :]
    ve, ue, dh, dx, div1, dx2, di2, uo, do, u_sems, d_sems = refs
    ni, depth = nv.shape[0], nv.shape[2] // LANES
    more_x = flags[1] > 0
    parts = (ni - 4) // PART

    def bound_of(p, j, s):
        return hb[p, j, 0:8, :] if s == 4 else tile(bv, p, j, s)

    def image_of(p, j, s):
        return hn[p, j, 0:8, :] if s == 4 else tile(nv, p, j, s)

    def di_of(p, j, s):
        return dh[p % 4, j, 0:8, :] if s == 4 else tile(di, p, j, s)

    t = Fields(
        lambda p: p % 4,
        bound_of=bound_of, image_of=image_of, di_of=di_of,
        dz_of=lambda p, j, s: tile(dz, p, j, s),
        ve=ve, ue=ue, dx=dx, div1=div1, dx2=dx2, di2=di2,
    )

    def writes(c):
        span = pl.ds(c * PART + 2, PART)
        return [pltpu.make_async_copy(uo.at[span], u_hbm.at[span], u_sems.at[c])] + [
            pltpu.make_async_copy(do.at[k, span], d_hbm.at[k, span], d_sems.at[k, c])
            for k in range(3)
        ]

    def hand(slots):
        for ref, (name, wanted) in zip(handed, HANDED):
            for slot in wanted:
                if slot not in slots:
                    continue
                plane = slot - 1 if slot < 4 else ni - 7 + slot
                for j in range(depth):
                    for s in range(4 if name in ("dz", "div1", "di2") else 5):
                        if name == "di":
                            value = di_of(plane, j, s)
                        elif name == "dz":
                            value = tile(dz, plane, j, s)
                        elif name in ("ve", "ue"):
                            value = getattr(t, name)[plane, j, strip(s), :]
                        else:
                            value = getattr(t, name)[plane % 4, j, strip(s), :]
                        ref[slot, j, strip(s), :] = value
                    if name in ("ve", "ue"):
                        behind = pl.ds(HALO + 8, 1)
                        ref[slot, j, behind, :] = getattr(t, name)[plane, j, behind, :]

    def ready(p):
        scale(p, depth, image_of, ve)

    def halo_i(p):
        return [
            clip(ve[p + 1, j, strip(4), :] - ve[p, j, strip(4), :], hb[p, j, 0:8, :])
            for j in range(depth)
        ]

    def first_inner(p, sums):
        p1, d1 = sums
        q = p % 4
        for s in (3,) + ORDER[:4]:
            v = [ve[p, j, strip(s), :] for j in range(depth)]
            b = [bound_of(p, j, s) for j in range(depth)]
            c = [-k for k in b]
            x = x_dual(p, s, depth, ve, v, b, c)
            for j in range(depth):
                dx[q, j, strip(s), :] = x[j]
            if s == 3:
                continue
            finish = [x[j] - dx[q, j, strip_back(s), :] for j in range(depth)]
            if s == 4:
                z = [clip2(n - o, k, m) for n, o, k, m in zip(depth_next(v), v, b, c)]
                back = depth_back(z)
                new = halo_i(p)
                for j in range(depth):
                    below = new[j] - dh[(p - 1) % 4, j, 0:8, :]
                    dh[q, j, 0:8, :] = new[j]
                    total = finish[j] + (z[j] - back[j]) + below
                    ue[p, j, strip(4), :] = v[j] + TWO_CS * total
                    dx[q, j, pl.ds(OWN - 1, 1), :] = dx[q, j, pl.ds(HALO + 7, 1), :]
                continue
            for j in range(depth):
                total = finish[j] + tile(part, p, j, s)
                ue[p, j, strip(s), :] = v[j] + TWO_CS * total
                div1[q, j, strip(s), :] = total
                p1 = p1 + total * total
                d1 = d1 + x[j] * x[j]
        s = 3
        for j in range(depth):
            x3 = dx[q, j, strip(s), :]
            total = (x3 - dx[q, j, strip_back(s), :]) + tile(part, p, j, s)
            ue[p, j, strip(s), :] = ve[p, j, strip(s), :] + TWO_CS * total
            div1[q, j, strip(s), :] = total
            p1 = p1 + total * total
            d1 = d1 + x3 * x3
        for j in range(depth):
            edge = ue[p, j, pl.ds(HALO - 1, 1), :]
            ue[p, j, pl.ds(HALO, 1), :] = jnp.where(more_x, ue[p, j, pl.ds(HALO, 1), :], edge)
        wrap_rows(ue, p, depth)
        return p1, d1

    for p in range(4):
        ready(p)
    for j, value in enumerate(halo_i(0)):
        dh[0, j, 0:8, :] = value
    zero = jnp.zeros((8, LANES), F32)
    a = first_inner(1, (zero, own_sum[...]))
    a = first_inner(2, a)
    for s in range(4):
        for j in range(depth):
            second_i(t, 1, s, j)
    hand((1, 2, 3))

    def body(p, carry):
        a, b = carry
        ready(p + 1)
        a = first_inner(p, a)
        b = second(t, p - 1, p - 1, depth, b, uo, do)

        @pl.when(p % PART == 0)
        def _():
            for copy in writes(p // PART - 2):
                copy.start()

        return a, b

    a, b = lax.fori_loop(3, ni - 1, body, (a, (zero, zero)))
    hand((4, 5, 6))
    for k, total in enumerate(a + b):
        sums_ref[k] = total
    for c in range(parts):
        for copy in writes(c):
            copy.wait()


def inner(flags, nv, bv, di, dz, part, own_sum, halo_n, halo_b):
    ni, nx, nz = nv.shape
    depth = nz // LANES
    full = pltpu.VMEM((ni, depth, ROWS, LANES), F32)
    short = pltpu.VMEM((4, depth, ROWS, LANES), F32)
    parts = (ni - 4) // PART
    slots = pltpu.VMEM((8, depth, ROWS, LANES), F32)
    return pl.pallas_call(
        inner_kernel,
        out_shape=(
            jax.ShapeDtypeStruct((ni, nx, nz), F32),
            jax.ShapeDtypeStruct((3, ni, nx, nz), F32),
            pltpu.VMEM((4, 8, LANES), F32),
        )
        + (slots,) * len(HANDED),
        in_specs=[pl.BlockSpec(memory_space=pltpu.SMEM)] + [pl.BlockSpec(memory_space=VMEM)] * 8,
        out_specs=[pl.BlockSpec(memory_space=HBM)] * 2
        + [pl.BlockSpec(memory_space=VMEM)] * (1 + len(HANDED)),
        scratch_shapes=[full] * 2
        + [pltpu.VMEM((4, depth, 8, LANES), F32)]
        + [short] * 4
        + [
            pltpu.VMEM((ni, nx, nz), F32),
            pltpu.VMEM((3, ni, nx, nz), F32),
            pltpu.SemaphoreType.DMA((parts,)),
            pltpu.SemaphoreType.DMA((3, parts)),
        ],
        compiler_params=pltpu.CompilerParams(vmem_limit_bytes=24 << 20),
        cost_estimate=pl.CostEstimate(flops=200_000_000, transcendentals=0, bytes_accessed=12 << 20),
        name="inner_planes",
    )(flags, nv, bv, di, dz, part, own_sum, halo_n, halo_b)


def edge_kernel(flags, got_a, got_c, n4_ref, b4_ref, hb, sums_ref, *refs):
    given = dict(zip([name for name, _ in HANDED], refs))
    refs = refs[len(HANDED) :]
    _, _, u_hbm, d_hbm, spread_ref = refs[:5]
    ve, ue, di, dx, dz, div1, di2, dx2, uo, do, u_sems, d_sems = refs[5:]
    own = dict(ve=ve, ue=ue, di=di, dx=dx, dz=dz, div1=div1, di2=di2)
    depth, ni = got_a.shape[0], u_hbm.shape[0]
    more_i, more_x, even_i = flags[0] > 0, flags[1] > 0, flags[2] == 0

    def up(j, row):
        rows = pl.ds(row, 8)
        return jnp.where(even_i, got_c[j, rows, :], got_a[j, rows, :])

    def down(j, row):
        rows = pl.ds(row, 8)
        return jnp.where(even_i, got_a[j, rows, :], got_c[j, rows, :])

    def bound_of(p, j, s):
        if p == 0:
            return up(j, 40 + 8 * s)
        return hb[boundary_planes(ni)[KEPT[p]], j, 0:8, :] if s == 4 else tile(b4_ref, KEPT[p], j, s)

    t = Fields(
        lambda p: p,
        dx2=dx2,
        bound_of=bound_of,
        image_of=lambda p, j, s: tile(n4_ref, KEPT[p], j, s),
        di_of=lambda p, j, s: t.di[p, j, strip(s), :],
        dz_of=lambda p, j, s: t.dz[p, j, strip(s), :],
        **{name: Split(given[name], own[name], slots) for name, slots in HANDED},
    )
    a = sums_ref[0], sums_ref[1]
    b = sums_ref[2], sums_ref[3]

    for j in range(depth):
        for s in range(5):
            t.ve[0, j, strip(s), :] = SIGMA * up(j, 8 * s)
            t.ve[7, j, strip(s), :] = jnp.where(
                more_i, SIGMA * down(j, 8 * s), t.ve[6, j, strip(s), :]
            )
    for j in range(depth):
        for s in range(5):
            low = clip(t.ve[1, j, strip(s), :] - t.ve[0, j, strip(s), :], up(j, 40 + 8 * s))
            t.di[0, j, strip(s), :] = low
            if s < 4:
                part = up(j, 80 + 8 * s)
                t.ue[0, j, strip(s), :] = t.ve[0, j, strip(s), :] + TWO_CS * (part + low)
    a = first(t, 1, depth, more_x, a)
    for s in range(4):
        for j in range(depth):
            second_i(t, 0, s, j)
    b = second(t, 1, 0, depth, b, uo, do)
    b = second(t, 2, 1, depth, b, uo, do)

    def writes(k, plane):
        at, to = pl.ds(2 * k, 2), pl.ds(plane, 2)
        return [pltpu.make_async_copy(uo.at[at], u_hbm.at[to], u_sems.at[k])] + [
            pltpu.make_async_copy(do.at[c, at], d_hbm.at[c, to], d_sems.at[c, k]) for c in range(3)
        ]

    copies = writes(0, 0)
    for copy in copies:
        copy.start()
    a = first(t, 6, depth, more_x, a)
    for j in range(depth):
        for s in range(4):
            part = down(j, 40 + 8 * s)
            top = t.ve[7, j, strip(s), :] + TWO_CS * (part - t.di[6, j, strip(s), :])
            t.ue[7, j, strip(s), :] = jnp.where(more_i, top, t.ue[6, j, strip(s), :])
    b = second(t, 5, 2, depth, b, uo, do)
    b = second(t, 6, 3, depth, b, uo, do)
    last = writes(1, ni - 2)
    for copy in last:
        copy.start()
    factors = (C * C, 1.0, C * C, 1.0)
    lane = lax.broadcasted_iota(jnp.int32, (1, 4), 1)
    row = jnp.zeros((1, 4), F32)
    for k, total in enumerate(a + b):
        row = jnp.where(lane == k, factors[k] * jnp.sum(total), row)
    spread_ref[...] = jnp.broadcast_to(row, spread_ref.shape)
    for copy in copies + last:
        copy.wait()


def edges(flags, got_a, got_c, n4, b4, halo_b, sums, handed, primal, dual, devices):
    _, nx, nz = primal.shape
    depth = nz // LANES
    buffer = pltpu.VMEM((8, depth, ROWS, LANES), F32)
    count = 7 + len(handed)
    return pl.pallas_call(
        edge_kernel,
        out_shape=(
            jax.ShapeDtypeStruct(primal.shape, F32),
            jax.ShapeDtypeStruct(dual.shape, F32),
            jax.ShapeDtypeStruct((devices, 4), F32),
        ),
        in_specs=[pl.BlockSpec(memory_space=pltpu.SMEM)]
        + [pl.BlockSpec(memory_space=VMEM)] * (count - 1)
        + [pl.BlockSpec(memory_space=HBM)] * 2,
        out_specs=[pl.BlockSpec(memory_space=HBM)] * 2 + [pl.BlockSpec(memory_space=VMEM)],
        scratch_shapes=[buffer] * 8
        + [
            pltpu.VMEM((4, nx, nz), F32),
            pltpu.VMEM((3, 4, nx, nz), F32),
            pltpu.SemaphoreType.DMA((2,)),
            pltpu.SemaphoreType.DMA((3, 2)),
        ],
        input_output_aliases={count: 0, count + 1: 1},
        compiler_params=pltpu.CompilerParams(vmem_limit_bytes=24 << 20),
        name="edge_planes",
    )(flags, got_a, got_c, n4, b4, halo_b, sums, *handed, primal, dual)


def per_device(noisy, bound):
    count_i, count_x = lax.axis_size("inl"), lax.axis_size("xln")
    at_i, at_x = lax.axis_index("inl"), lax.axis_index("xln")
    flags = jnp.stack(
        [
            (at_i < count_i - 1).astype(jnp.int32),
            (at_x < count_x - 1).astype(jnp.int32),
            at_i % 2,
            at_x % 2,
        ]
    )
    noisy, bound = (pltpu.with_memory_space_constraint(x, HBM) for x in (noisy, bound))
    send_a, send_c, n4, b4 = pack(flags, noisy, bound)
    got_c = swapped(send_c, "xln", 1)
    got_a = swapped(send_a, "xln", 0)
    alone = own(noisy, bound)
    face_a, face_c, halo_n, halo_b = planes(
        flags, n4, b4, send_a, send_c, got_a, got_c, alone[-1]
    )
    back_a = swapped(face_a, "inl", 0)
    back_c = swapped(face_c, "inl", 1)
    primal, dual, sums, *handed = inner(flags, *alone, halo_n, halo_b)
    primal, dual, spread = edges(
        flags, back_a, back_c, n4, b4, halo_b, sums, handed, primal, dual, count_i * count_x
    )
    parts = lax.all_to_all(spread, AXES, 0, 0, tiled=True)
    norms = jnp.sqrt(jnp.sum(parts, axis=0)).reshape(2, 2)
    return primal, dual, norms


def solution(mesh):
    in_specs = (P("inl", "xln", None), P("inl", "xln", None))
    out_specs = (P("inl", "xln", None), P(None, "inl", "xln", None), P())
    return jax.shard_map(
        per_device, mesh=mesh, in_specs=in_specs, out_specs=out_specs, check_vma=False
    )
```

```python
import jax
import jax.numpy as jnp
from jax import lax
from jax.experimental import pallas as pl
from jax.experimental.pallas import tpu as pltpu
from jax.sharding import PartitionSpec as P

SIGMA = 0.28
TAU = 0.28
C = TAU / (1.0 + TAU)
C_OLD = C / (1.0 + TAU)
TWO_CS = 2.0 * C * SIGMA

LANES = 128
ROWS = 56
OWN = 8
HALO = 40
AXES = ("inl", "xln")
F32 = jnp.float32


def swapped(value, axis, first):
    count = lax.axis_size(axis)
    pairs = []
    for low in range(first, count - 1, 2):
        pairs += [(low, low + 1), (low + 1, low)]
    return lax.ppermute(value, axis, pairs)


def place():
    i, x = lax.axis_index("inl"), lax.axis_index("xln")
    more_i = i < lax.axis_size("inl") - 1
    more_x = x < lax.axis_size("xln") - 1
    return more_i, more_x, lax.rem(i, 2) == 0, lax.rem(x, 2) == 0


def clip(value, bound):
    return jnp.minimum(jnp.maximum(value, -bound), bound)


def last_lane():
    return lax.broadcasted_iota(jnp.int32, (8, LANES), 1) == LANES - 1


def first_lane():
    return lax.broadcasted_iota(jnp.int32, (8, LANES), 1) == 0


def depth_next(tiles):
    rolled = [pltpu.roll(t, LANES - 1, 1) for t in tiles] + [tiles[-1]]
    mask = last_lane()
    return [jnp.where(mask, rolled[j + 1], rolled[j]) for j in range(len(tiles))]


def depth_back(tiles):
    rolled = [jnp.zeros((8, LANES), F32)] + [pltpu.roll(t, 1, 1) for t in tiles]
    mask = first_lane()
    return [jnp.where(mask, rolled[j], rolled[j + 1]) for j in range(len(tiles))]


def pack_kernel(n_hbm, b_hbm, a_ref, c_ref, n4_ref, b4_ref, slab, sems, plane_sems):
    ni, nx, depth = n_hbm.shape[0], n_hbm.shape[1], n_hbm.shape[2] // LANES
    even = place()[3]
    columns, planes = [], []
    for k, src in enumerate((n_hbm, b_hbm)):
        for m, start in enumerate((nx - 2, 0)):
            columns.append(
                pltpu.make_async_copy(src.at[:, pl.ds(start, 2), :], slab.at[m, k], sems.at[m, k])
            )
    for k, (src, dst) in enumerate(((n_hbm, n4_ref), (b_hbm, b4_ref))):
        for q, i in enumerate((0, ni - 2)):
            planes.append(
                pltpu.make_async_copy(
                    src.at[pl.ds(i, 2)], dst.at[pl.ds(2 * q, 2)], plane_sems.at[k, q]
                )
            )
    for c in columns + planes:
        c.start()
    for c in columns:
        c.wait()

    def body(i, _):
        for k in range(2):
            for j in range(depth):
                lanes = pl.ds(j * LANES, LANES)
                high, low = slab[0, k, i, 0:2, lanes], slab[1, k, i, 0:2, lanes]
                a_ref[i, j, 2 * k : 2 * k + 2, :] = jnp.where(even, high, low)
                c_ref[i, j, 2 * k : 2 * k + 2, :] = jnp.where(even, low, high)
        return 0

    lax.fori_loop(0, ni, body, 0, unroll=2)
    for c in planes:
        c.wait()


HBM = pltpu.MemorySpace.HBM
VMEM = pltpu.MemorySpace.VMEM


def pack(noisy, bound):
    ni, nx, nz = noisy.shape
    depth = nz // LANES
    message = pltpu.VMEM((ni, depth, 4, LANES), F32)
    boundary = pltpu.VMEM((4, nx, nz), F32)
    return pl.pallas_call(
        pack_kernel,
        out_shape=(message, message, boundary, boundary),
        in_specs=[pl.BlockSpec(memory_space=HBM)] * 2,
        out_specs=[pl.BlockSpec(memory_space=VMEM)] * 4,
        scratch_shapes=[
            pltpu.VMEM((2, 2, ni, 2, nz), F32),
            pltpu.SemaphoreType.DMA((2, 2)),
            pltpu.SemaphoreType.DMA((2, 2)),
        ],
        compiler_params=pltpu.CompilerParams(vmem_limit_bytes=8 << 20),
        name="pack_faces",
    )(noisy, bound)


def strip(s):
    return pl.ds(OWN + 8 * s, 8)


def strip_next(s):
    return pl.ds(OWN + 8 * s + 1, 8)


def strip_back(s):
    return pl.ds(OWN + 8 * s - 1, 8)


def wrap_rows(field, p, depth):
    for j in range(depth):
        field[p, j, pl.ds(HALO + 8, 1), :] = field[p, j, pl.ds(OWN, 1), :]


def scale(p, depth, image_of, ve):
    for j in range(depth):
        for s in range(5):
            ve[p, j, strip(s), :] = SIGMA * image_of(p, j, s)
    wrap_rows(ve, p, depth)


def tile(field, p, j, s):
    return field[p, pl.ds(8 * s, 8), pl.ds(j * LANES, LANES)]


def x_dual(p, s, depth, ve, v, b, c):
    return [
        clip2(ve[p, j, strip_next(s), :] - v[j], b[j], c[j]) for j in range(depth)
    ]


def clip2(value, bound, below):
    return jnp.minimum(jnp.maximum(value, below), bound)


ORDER = (4, 0, 1, 2, 3)


def crossline(p, q, depth, ve, bound_of, dx, then):
    for s in (3,) + ORDER:
        v = [ve[p, j, strip(s), :] for j in range(depth)]
        b = [bound_of(p, j, s) for j in range(depth)]
        c = [-k for k in b]
        x = x_dual(p, s, depth, ve, v, b, c)
        for j in range(depth):
            dx[q, j, strip(s), :] = x[j]
        if s == 3:
            break
    for s in ORDER:
        v = [ve[p, j, strip(s), :] for j in range(depth)]
        b = [bound_of(p, j, s) for j in range(depth)]
        c = [-k for k in b]
        if s == 3:
            x = [dx[q, j, strip(s), :] for j in range(depth)]
        else:
            x = x_dual(p, s, depth, ve, v, b, c)
            for j in range(depth):
                dx[q, j, strip(s), :] = x[j]
        z = [clip2(n - o, k, m) for n, o, k, m in zip(depth_next(v), v, b, c)]
        back = depth_back(z)
        div = [x[j] - dx[q, j, strip_back(s), :] + (z[j] - back[j]) for j in range(depth)]
        then(s, v, b, c, x, z, div)
        if s == 4:
            for j in range(depth):
                dx[q, j, pl.ds(OWN - 1, 1), :] = dx[q, j, pl.ds(HALO + 7, 1), :]


def planes_kernel(
    n4_ref, b4_ref, sent_a, sent_c, got_a, got_c, _,
    a_ref, c_ref, hn, hb, ve, dx,
):
    ni, depth = got_a.shape[0], got_a.shape[1]
    _, more_x, even_i, even_x = place()

    def sort(i, _):
        for j in range(depth):
            last = jnp.where(even_x, sent_a[i, j, 1:2, :], sent_c[i, j, 1:2, :])
            a_n, c_n = got_a[i, j, 0:2, :], got_c[i, j, 0:2, :]
            a_b, c_b = got_a[i, j, 2:4, :], got_c[i, j, 2:4, :]
            hn[i, j, 6:8, :] = jnp.where(even_x, c_n, a_n)
            hb[i, j, 6:8, :] = jnp.where(even_x, c_b, a_b)
            above = jnp.where(even_x, a_n, c_n)
            hn[i, j, 0:2, :] = above
            hb[i, j, 0:2, :] = jnp.where(even_x, a_b, c_b)
            hn[i, j, 0:1, :] = jnp.where(more_x, above[0:1], last)
        return 0

    lax.fori_loop(0, ni, sort, 0, unroll=2)
    planes_at = (0, 1, ni - 2, ni - 1)

    def image_of(q, j, s):
        return hn[planes_at[q], j, 0:8, :] if s == 4 else tile(n4_ref, q, j, s)

    def bound_of(q, j, s):
        return hb[planes_at[q], j, 0:8, :] if s == 4 else tile(b4_ref, q, j, s)

    for q in range(4):
        scale(q, depth, image_of, ve)

    def up(ref):
        for s in range(5):
            for j in range(depth):
                ref[j, pl.ds(8 * s, 8), :] = image_of(3, j, s)
                ref[j, pl.ds(40 + 8 * s, 8), :] = bound_of(3, j, s)

        def then(s, v, b, c, x, z, div):
            if s == 4:
                return
            for j in range(depth):
                before = clip(v[j] - ve[2, j, strip(s), :], bound_of(2, j, s))
                ref[j, pl.ds(80 + 8 * s, 8), :] = div[j] - before

        crossline(3, 3, depth, ve, bound_of, dx, then)

    def down(ref):
        for s in range(5):
            for j in range(depth):
                ref[j, pl.ds(8 * s, 8), :] = image_of(0, j, s)

        def then(s, v, b, c, x, z, div):
            if s == 4:
                return
            for j in range(depth):
                own = clip2(ve[1, j, strip(s), :] - v[j], b[j], c[j])
                ref[j, pl.ds(40 + 8 * s, 8), :] = div[j] + own

        crossline(0, 0, depth, ve, bound_of, dx, then)

    @pl.when(even_i)
    def _():
        up(a_ref)
        down(c_ref)

    @pl.when(jnp.logical_not(even_i))
    def _():
        down(a_ref)
        up(c_ref)


def planes(n4, b4, sent_a, sent_c, got_a, got_c, after):
    ni, depth = got_a.shape[0], got_a.shape[1]
    buffer = pltpu.VMEM((4, depth, ROWS, LANES), F32)
    return pl.pallas_call(
        planes_kernel,
        out_shape=(pltpu.VMEM((depth, 112, LANES), F32),) * 2
        + (pltpu.VMEM((ni, depth, 8, LANES), F32),) * 2,
        in_specs=[pl.BlockSpec(memory_space=VMEM)] * 7,
        out_specs=[pl.BlockSpec(memory_space=VMEM)] * 4,
        scratch_shapes=[buffer] * 2,
        compiler_params=pltpu.CompilerParams(vmem_limit_bytes=8 << 20),
        name="pack_planes",
    )(n4, b4, sent_a, sent_c, got_a, got_c, after)


class Fields:
    def __init__(self, ring, **fields):
        self.ring = ring
        self.__dict__.update(fields)


class Split:
    def __init__(self, given, own, slots):
        self.given, self.own, self.slots = given, own, slots

    def __getitem__(self, index):
        return (self.given if index[0] in self.slots else self.own)[index]

    def __setitem__(self, index, value):
        self.own[index] = value


def first(t, p, depth, more_x, sums):
    sums = list(sums)
    q, before = t.ring(p), t.ring(p - 1)

    def then(s, v, b, c, x, z, div):
        for j in range(depth):
            i_new = clip2(t.ve[p + 1, j, strip(s), :] - v[j], b[j], c[j])
            t.di[q, j, strip(s), :] = i_new
            total = div[j] + (i_new - t.di[before, j, strip(s), :])
            t.ue[p, j, strip(s), :] = v[j] + TWO_CS * total
            if s < 4:
                t.dz[q, j, strip(s), :] = z[j]
                t.div1[q, j, strip(s), :] = total
                sums[0] = sums[0] + total * total
                sums[1] = sums[1] + (x[j] * x[j] + (i_new * i_new + z[j] * z[j]))

    crossline(p, q, depth, t.ve, t.bound_of, t.dx, then)
    for j in range(depth):
        edge = t.ue[p, j, pl.ds(HALO - 1, 1), :]
        t.ue[p, j, pl.ds(HALO, 1), :] = jnp.where(more_x, t.ue[p, j, pl.ds(HALO, 1), :], edge)
    wrap_rows(t.ue, p, depth)
    return tuple(sums)


def second_i(t, p, s, j):
    q = t.ring(p)
    t.di2[q, j, strip(s), :] = clip(
        t.di_of(p, j, s) + (t.ue[p + 1, j, strip(s), :] - t.ue[p, j, strip(s), :]),
        t.bound_of(p, j, s),
    )


def second(t, p, o, depth, sums, uo, do):
    p2, d2 = sums
    q, before = t.ring(p), t.ring(p - 1)
    for s in ORDER:
        u = [t.ue[p, j, strip(s), :] for j in range(depth)]
        b = [t.bound_of(p, j, s) for j in range(depth)]
        c = [-k for k in b]
        x_old = [t.dx[q, j, strip(s), :] for j in range(depth)]
        x_new = [
            clip2(x_old[j] + (t.ue[p, j, strip_next(s), :] - u[j]), b[j], c[j])
            for j in range(depth)
        ]
        for j in range(depth):
            t.dx2[q, j, strip(s), :] = x_new[j]
        if s == 4:
            for j in range(depth):
                t.dx2[q, j, pl.ds(OWN - 1, 1), :] = t.dx2[q, j, pl.ds(HALO + 7, 1), :]
            continue
        z_old = [t.dz_of(p, j, s) for j in range(depth)]
        z_new = [
            clip2(z_old[j] + (n - u[j]), b[j], c[j]) for j, n in enumerate(depth_next(u))
        ]
        back = depth_back(z_new)
        rows = pl.ds(8 * s, 8)
        for j in range(depth):
            lanes = pl.ds(j * LANES, LANES)
            i_old = t.di_of(p, j, s)
            i_new = clip2(i_old + (t.ue[p + 1, j, strip(s), :] - u[j]), b[j], c[j])
            t.di2[q, j, strip(s), :] = i_new
            total = (
                (x_new[j] - t.dx2[q, j, strip_back(s), :])
                + (z_new[j] - back[j])
                + (i_new - t.di2[before, j, strip(s), :])
            )
            old = t.div1[q, j, strip(s), :]
            uo[o, rows, lanes] = t.image_of(p, j, s) + (C * total + C_OLD * old)
            do[0, o, rows, lanes] = i_new
            do[1, o, rows, lanes] = x_new[j]
            do[2, o, rows, lanes] = z_new[j]
            gap = total - C * old
            p2 = p2 + gap * gap
            gi = i_new - i_old
            gx = x_new[j] - x_old[j]
            gz = z_new[j] - z_old[j]
            d2 = d2 + (gi * gi + (gx * gx + gz * gz))
    return p2, d2


KEPT = {1: 0, 2: 1, 5: 2, 6: 3}


def boundary_planes(ni):
    return 0, 1, ni - 2, ni - 1


GROUP = 3
PART = 2
HANDED = (
    ("ve", (1, 2, 5, 6)),
    ("ue", (2, 3, 4, 5)),
    ("di", (2, 5)),
    ("dx", (2, 5)),
    ("dz", (2, 5)),
    ("div1", (2, 5)),
    ("di2", (4,)),
)


def own_kernel(n_hbm, b_hbm, nv, bv, di, dz, part, sum_ref, sems):
    ni, depth = n_hbm.shape[0], n_hbm.shape[2] // LANES
    steps = (ni - 2) // GROUP

    def reads(c, start, count):
        span = pl.ds(start, count)
        return [
            pltpu.make_async_copy(src.at[span], dst.at[span], sems.at[k, c])
            for k, (src, dst) in enumerate(((n_hbm, nv), (b_hbm, bv)))
        ]

    ahead = reads(0, 0, GROUP + 2)
    for copy in ahead:
        copy.start()
    for c in range(1, steps):
        for copy in reads(c, c * GROUP + 2, GROUP):
            copy.start()
    for copy in ahead:
        copy.wait()

    def spot(j, s):
        return pl.ds(8 * s, 8), pl.ds(j * LANES, LANES)

    for s in range(4):
        for j in range(depth):
            gap = SIGMA * (tile(nv, 1, j, s) - tile(nv, 0, j, s))
            di[(0,) + spot(j, s)] = clip(gap, tile(bv, 0, j, s))

    def body(step, total):
        @pl.when(step > 0)
        def _():
            for copy in reads(step, step * GROUP + 2, GROUP):
                copy.wait()

        for k in range(GROUP):
            p = step * GROUP + 1 + k
            for s in range(4):
                n = [tile(nv, p, j, s) for j in range(depth)]
                b = [tile(bv, p, j, s) for j in range(depth)]
                c = [-k for k in b]
                z = [clip2(SIGMA * (m - o), k, l) for m, o, k, l in zip(depth_next(n), n, b, c)]
                back = depth_back(z)
                for j in range(depth):
                    new = clip2(SIGMA * (tile(nv, p + 1, j, s) - n[j]), b[j], c[j])
                    at = (p,) + spot(j, s)
                    di[at] = new
                    dz[at] = z[j]
                    part[at] = (new - tile(di, p - 1, j, s)) + (z[j] - back[j])
                    total = total + (new * new + z[j] * z[j])
        return total

    sum_ref[0] = lax.fori_loop(0, steps, body, jnp.zeros((8, LANES), F32))


def own(noisy, bound):
    ni, nx, nz = noisy.shape
    whole = pltpu.VMEM((ni, nx, nz), F32)
    return pl.pallas_call(
        own_kernel,
        out_shape=(whole,) * 5 + (pltpu.VMEM((4, 8, LANES), F32),),
        in_specs=[pl.BlockSpec(memory_space=HBM)] * 2,
        out_specs=[pl.BlockSpec(memory_space=VMEM)] * 6,
        scratch_shapes=[pltpu.SemaphoreType.DMA((2, (ni - 2) // GROUP))],
        compiler_params=pltpu.CompilerParams(vmem_limit_bytes=16 << 20),
        cost_estimate=pl.CostEstimate(flops=100_000_000, transcendentals=0, bytes_accessed=4 << 20),
        name="own_planes",
    )(noisy, bound)


def inner_kernel(nv, bv, di, dz, part, own_sum, hn, hb, u_hbm, d_hbm, sums_ref, *refs):
    handed, refs = refs[: len(HANDED)], refs[len(HANDED) :]
    ve, ue, dh, dx, div1, dx2, di2, uo, do, u_sems, d_sems = refs
    ni, depth = nv.shape[0], nv.shape[2] // LANES
    more_x = place()[1]
    parts = (ni - 4) // PART

    def bound_of(p, j, s):
        return hb[p, j, 0:8, :] if s == 4 else tile(bv, p, j, s)

    def image_of(p, j, s):
        return hn[p, j, 0:8, :] if s == 4 else tile(nv, p, j, s)

    def di_of(p, j, s):
        return dh[p % 4, j, 0:8, :] if s == 4 else tile(di, p, j, s)

    t = Fields(
        lambda p: p % 4,
        bound_of=bound_of, image_of=image_of, di_of=di_of,
        dz_of=lambda p, j, s: tile(dz, p, j, s),
        ve=ve, ue=ue, dx=dx, div1=div1, dx2=dx2, di2=di2,
    )

    def writes(c):
        span = pl.ds(c * PART + 2, PART)
        return [pltpu.make_async_copy(uo.at[span], u_hbm.at[span], u_sems.at[c])] + [
            pltpu.make_async_copy(do.at[k, span], d_hbm.at[k, span], d_sems.at[k, c])
            for k in range(3)
        ]

    def hand(slots):
        for ref, (name, wanted) in zip(handed, HANDED):
            for slot in wanted:
                if slot not in slots:
                    continue
                plane = slot - 1 if slot < 4 else ni - 7 + slot
                for j in range(depth):
                    for s in range(4 if name in ("dz", "div1", "di2") else 5):
                        if name == "di":
                            value = di_of(plane, j, s)
                        elif name == "dz":
                            value = tile(dz, plane, j, s)
                        elif name in ("ve", "ue"):
                            value = getattr(t, name)[plane, j, strip(s), :]
                        else:
                            value = getattr(t, name)[plane % 4, j, strip(s), :]
                        ref[slot, j, strip(s), :] = value
                    if name in ("ve", "ue"):
                        behind = pl.ds(HALO + 8, 1)
                        ref[slot, j, behind, :] = getattr(t, name)[plane, j, behind, :]

    def ready(p):
        scale(p, depth, image_of, ve)

    def halo_i(p):
        return [
            clip(ve[p + 1, j, strip(4), :] - ve[p, j, strip(4), :], hb[p, j, 0:8, :])
            for j in range(depth)
        ]

    def first_inner(p, sums):
        p1, d1 = sums
        q = p % 4
        for s in (3,) + ORDER[:4]:
            v = [ve[p, j, strip(s), :] for j in range(depth)]
            b = [bound_of(p, j, s) for j in range(depth)]
            c = [-k for k in b]
            x = x_dual(p, s, depth, ve, v, b, c)
            for j in range(depth):
                dx[q, j, strip(s), :] = x[j]
            if s == 3:
                continue
            finish = [x[j] - dx[q, j, strip_back(s), :] for j in range(depth)]
            if s == 4:
                z = [clip2(n - o, k, m) for n, o, k, m in zip(depth_next(v), v, b, c)]
                back = depth_back(z)
                new = halo_i(p)
                for j in range(depth):
                    below = new[j] - dh[(p - 1) % 4, j, 0:8, :]
                    dh[q, j, 0:8, :] = new[j]
                    total = finish[j] + (z[j] - back[j]) + below
                    ue[p, j, strip(4), :] = v[j] + TWO_CS * total
                    dx[q, j, pl.ds(OWN - 1, 1), :] = dx[q, j, pl.ds(HALO + 7, 1), :]
                continue
            for j in range(depth):
                total = finish[j] + tile(part, p, j, s)
                ue[p, j, strip(s), :] = v[j] + TWO_CS * total
                div1[q, j, strip(s), :] = total
                p1 = p1 + total * total
                d1 = d1 + x[j] * x[j]
        s = 3
        for j in range(depth):
            x3 = dx[q, j, strip(s), :]
            total = (x3 - dx[q, j, strip_back(s), :]) + tile(part, p, j, s)
            ue[p, j, strip(s), :] = ve[p, j, strip(s), :] + TWO_CS * total
            div1[q, j, strip(s), :] = total
            p1 = p1 + total * total
            d1 = d1 + x3 * x3
        for j in range(depth):
            edge = ue[p, j, pl.ds(HALO - 1, 1), :]
            ue[p, j, pl.ds(HALO, 1), :] = jnp.where(more_x, ue[p, j, pl.ds(HALO, 1), :], edge)
        wrap_rows(ue, p, depth)
        return p1, d1

    for p in range(4):
        ready(p)
    for j, value in enumerate(halo_i(0)):
        dh[0, j, 0:8, :] = value
    zero = jnp.zeros((8, LANES), F32)
    a = first_inner(1, (zero, own_sum[0]))
    a = first_inner(2, a)
    for s in range(4):
        for j in range(depth):
            second_i(t, 1, s, j)
    hand((1, 2, 3))

    def body(step, carry):
        a, b = carry
        for k in range(PART):
            p = step * PART + 3 + k
            ready(p + 1)
            a = first_inner(p, a)
            b = second(t, p - 1, p - 1, depth, b, uo, do)
        for copy in writes(step):
            copy.start()
        return a, b

    a, b = lax.fori_loop(0, parts, body, (a, (zero, zero)))
    hand((4, 5, 6))
    for k, total in enumerate(a + b):
        sums_ref[k] = total
    for c in range(parts):
        for copy in writes(c):
            copy.wait()


def inner(nv, bv, di, dz, part, own_sum, halo_n, halo_b):
    ni, nx, nz = nv.shape
    depth = nz // LANES
    full = pltpu.VMEM((ni, depth, ROWS, LANES), F32)
    short = pltpu.VMEM((4, depth, ROWS, LANES), F32)
    parts = (ni - 4) // PART
    slots = pltpu.VMEM((8, depth, ROWS, LANES), F32)
    return pl.pallas_call(
        inner_kernel,
        out_shape=(
            jax.ShapeDtypeStruct((ni, nx, nz), F32),
            jax.ShapeDtypeStruct((3, ni, nx, nz), F32),
            pltpu.VMEM((4, 8, LANES), F32),
        )
        + (slots,) * len(HANDED),
        in_specs=[pl.BlockSpec(memory_space=VMEM)] * 8,
        out_specs=[pl.BlockSpec(memory_space=HBM)] * 2
        + [pl.BlockSpec(memory_space=VMEM)] * (1 + len(HANDED)),
        scratch_shapes=[full] * 2
        + [pltpu.VMEM((4, depth, 8, LANES), F32)]
        + [short] * 4
        + [
            pltpu.VMEM((ni, nx, nz), F32),
            pltpu.VMEM((3, ni, nx, nz), F32),
            pltpu.SemaphoreType.DMA((parts,)),
            pltpu.SemaphoreType.DMA((3, parts)),
        ],
        compiler_params=pltpu.CompilerParams(vmem_limit_bytes=24 << 20),
        cost_estimate=pl.CostEstimate(flops=200_000_000, transcendentals=0, bytes_accessed=12 << 20),
        name="inner_planes",
    )(nv, bv, di, dz, part, own_sum, halo_n, halo_b)


def edge_kernel(got_a, got_c, n4_ref, b4_ref, hb, sums_ref, *refs):
    given = dict(zip([name for name, _ in HANDED], refs))
    refs = refs[len(HANDED) :]
    _, _, u_hbm, d_hbm, spread_ref = refs[:5]
    ve, ue, di, dx, dz, div1, di2, dx2, uo, do, u_sems, d_sems = refs[5:]
    own = dict(ve=ve, ue=ue, di=di, dx=dx, dz=dz, div1=div1, di2=di2)
    depth, ni = got_a.shape[0], u_hbm.shape[0]
    more_i, more_x, even_i, _ = place()

    def up(j, row):
        rows = pl.ds(row, 8)
        return jnp.where(even_i, got_c[j, rows, :], got_a[j, rows, :])

    def down(j, row):
        rows = pl.ds(row, 8)
        return jnp.where(even_i, got_a[j, rows, :], got_c[j, rows, :])

    def bound_of(p, j, s):
        if p == 0:
            return up(j, 40 + 8 * s)
        return hb[boundary_planes(ni)[KEPT[p]], j, 0:8, :] if s == 4 else tile(b4_ref, KEPT[p], j, s)

    t = Fields(
        lambda p: p,
        dx2=dx2,
        bound_of=bound_of,
        image_of=lambda p, j, s: tile(n4_ref, KEPT[p], j, s),
        di_of=lambda p, j, s: t.di[p, j, strip(s), :],
        dz_of=lambda p, j, s: t.dz[p, j, strip(s), :],
        **{name: Split(given[name], own[name], slots) for name, slots in HANDED},
    )
    a = sums_ref[0], sums_ref[1]
    b = sums_ref[2], sums_ref[3]

    for j in range(depth):
        for s in range(5):
            t.ve[0, j, strip(s), :] = SIGMA * up(j, 8 * s)
            t.ve[7, j, strip(s), :] = jnp.where(
                more_i, SIGMA * down(j, 8 * s), t.ve[6, j, strip(s), :]
            )
    for j in range(depth):
        for s in range(5):
            low = clip(t.ve[1, j, strip(s), :] - t.ve[0, j, strip(s), :], up(j, 40 + 8 * s))
            t.di[0, j, strip(s), :] = low
            if s < 4:
                part = up(j, 80 + 8 * s)
                t.ue[0, j, strip(s), :] = t.ve[0, j, strip(s), :] + TWO_CS * (part + low)
    a = first(t, 1, depth, more_x, a)
    for s in range(4):
        for j in range(depth):
            second_i(t, 0, s, j)
    b = second(t, 1, 0, depth, b, uo, do)
    b = second(t, 2, 1, depth, b, uo, do)

    def writes(k, plane):
        at, to = pl.ds(2 * k, 2), pl.ds(plane, 2)
        return [pltpu.make_async_copy(uo.at[at], u_hbm.at[to], u_sems.at[k])] + [
            pltpu.make_async_copy(do.at[c, at], d_hbm.at[c, to], d_sems.at[c, k]) for c in range(3)
        ]

    copies = writes(0, 0)
    for copy in copies:
        copy.start()
    a = first(t, 6, depth, more_x, a)
    for j in range(depth):
        for s in range(4):
            part = down(j, 40 + 8 * s)
            top = t.ve[7, j, strip(s), :] + TWO_CS * (part - t.di[6, j, strip(s), :])
            t.ue[7, j, strip(s), :] = jnp.where(more_i, top, t.ue[6, j, strip(s), :])
    b = second(t, 5, 2, depth, b, uo, do)
    b = second(t, 6, 3, depth, b, uo, do)
    last = writes(1, ni - 2)
    for copy in last:
        copy.start()
    factors = (C * C, 1.0, C * C, 1.0)
    lane = lax.broadcasted_iota(jnp.int32, (1, 4), 1)
    row = jnp.zeros((1, 4), F32)
    for k, total in enumerate(a + b):
        row = jnp.where(lane == k, factors[k] * jnp.sum(total), row)
    spread_ref[...] = jnp.broadcast_to(row, spread_ref.shape)
    for copy in copies + last:
        copy.wait()


def edges(got_a, got_c, n4, b4, halo_b, sums, handed, primal, dual, devices):
    _, nx, nz = primal.shape
    depth = nz // LANES
    buffer = pltpu.VMEM((8, depth, ROWS, LANES), F32)
    count = 6 + len(handed)
    return pl.pallas_call(
        edge_kernel,
        out_shape=(
            jax.ShapeDtypeStruct(primal.shape, F32),
            jax.ShapeDtypeStruct(dual.shape, F32),
            jax.ShapeDtypeStruct((devices, 4), F32),
        ),
        in_specs=[pl.BlockSpec(memory_space=VMEM)] * count
        + [pl.BlockSpec(memory_space=HBM)] * 2,
        out_specs=[pl.BlockSpec(memory_space=HBM)] * 2 + [pl.BlockSpec(memory_space=VMEM)],
        scratch_shapes=[buffer] * 8
        + [
            pltpu.VMEM((4, nx, nz), F32),
            pltpu.VMEM((3, 4, nx, nz), F32),
            pltpu.SemaphoreType.DMA((2,)),
            pltpu.SemaphoreType.DMA((3, 2)),
        ],
        input_output_aliases={count: 0, count + 1: 1},
        compiler_params=pltpu.CompilerParams(vmem_limit_bytes=24 << 20),
        name="edge_planes",
    )(got_a, got_c, n4, b4, halo_b, sums, *handed, primal, dual)


def per_device(noisy, bound):
    count_i, count_x = lax.axis_size("inl"), lax.axis_size("xln")
    noisy, bound = (pltpu.with_memory_space_constraint(x, HBM) for x in (noisy, bound))
    send_a, send_c, n4, b4 = pack(noisy, bound)
    got_c = swapped(send_c, "xln", 1)
    got_a = swapped(send_a, "xln", 0)
    alone = own(noisy, bound)
    face_a, face_c, halo_n, halo_b = planes(
        n4, b4, send_a, send_c, got_a, got_c, alone[-1]
    )
    back_a = swapped(face_a, "inl", 0)
    back_c = swapped(face_c, "inl", 1)
    primal, dual, sums, *handed = inner(*alone, halo_n, halo_b)
    primal, dual, spread = edges(
        back_a, back_c, n4, b4, halo_b, sums, handed, primal, dual, count_i * count_x
    )
    parts = lax.all_to_all(spread, AXES, 0, 0, tiled=True)
    norms = jnp.sqrt(jnp.sum(parts, axis=0)).reshape(2, 2)
    return primal, dual, norms


def solution(mesh):
    in_specs = (P("inl", "xln", None), P("inl", "xln", None))
    out_specs = (P("inl", "xln", None), P(None, "inl", "xln", None), P())
    return jax.shard_map(
        per_device, mesh=mesh, in_specs=in_specs, out_specs=out_specs, check_vma=False
    )
```

```python
import jax
import jax.numpy as jnp
from jax import lax
from jax.experimental import pallas as pl
from jax.experimental.pallas import tpu as pltpu
from jax.sharding import PartitionSpec as P


SIGMA = 0.28
TAU = 0.28
C = TAU / (1.0 + TAU)
C_OLD = C / (1.0 + TAU)
TWO_CS = 2.0 * C * SIGMA
WIDE = 1e30

LANES = 128
ROWS = 56
OWN = 8
HALO = 40
AXES = ("inl", "xln")
F32 = jnp.float32


def swapped(value, axis, first):
    count = lax.axis_size(axis)
    pairs = []
    for low in range(first, count - 1, 2):
        pairs += [(low, low + 1), (low + 1, low)]
    return lax.ppermute(value, axis, pairs)


def place():
    i, x = lax.axis_index("inl"), lax.axis_index("xln")
    more_i = i < lax.axis_size("inl") - 1
    more_x = x < lax.axis_size("xln") - 1
    return more_i, more_x, lax.rem(i, 2) == 0, lax.rem(x, 2) == 0


def clip(value, bound):
    return jnp.minimum(jnp.maximum(value, -bound), bound)


def last_lane():
    return lax.broadcasted_iota(jnp.int32, (8, LANES), 1) == LANES - 1


def first_lane():
    return lax.broadcasted_iota(jnp.int32, (8, LANES), 1) == 0


def depth_next(tiles):
    rolled = [pltpu.roll(t, LANES - 1, 1) for t in tiles] + [tiles[-1]]
    mask = last_lane()
    return [jnp.where(mask, rolled[j + 1], rolled[j]) for j in range(len(tiles))]


def depth_back(tiles):
    rolled = [jnp.zeros((8, LANES), F32)] + [pltpu.roll(t, 1, 1) for t in tiles]
    mask = first_lane()
    return [jnp.where(mask, rolled[j], rolled[j + 1]) for j in range(len(tiles))]


def pack_kernel(n_hbm, b_hbm, a_ref, c_ref, n4_ref, b4_ref, slab, sems, plane_sems):
    ni, nx, depth = n_hbm.shape[0], n_hbm.shape[1], n_hbm.shape[2] // LANES
    even = place()[3]
    columns, planes = [], []
    for k, src in enumerate((n_hbm, b_hbm)):
        for m, x in enumerate((nx - 2, nx - 1, 0, 1)):
            columns.append(
                pltpu.make_async_copy(src.at[:, x, :], slab.at[m, k], sems.at[m, k])
            )
    for k, (src, dst) in enumerate(((n_hbm, n4_ref), (b_hbm, b4_ref))):
        for q, i in enumerate((0, ni - 2)):
            planes.append(
                pltpu.make_async_copy(
                    src.at[pl.ds(i, 2)], dst.at[pl.ds(2 * q, 2)], plane_sems.at[k, q]
                )
            )
    for c in columns + planes:
        c.start()
    for c in columns:
        c.wait()

    for r in range(0, ni, 8):
        rows = pl.ds(r, 8)
        n = [slab[m, 0, rows, :] for m in range(4)]
        b = [slab[m, 1, rows, :] for m in range(3)]
        high = n[1], b[1], clip(SIGMA * (n[1] - n[0]), b[0])
        low = n[2], b[2], clip(SIGMA * (n[3] - n[2]), b[2])
        for k, (h, l) in enumerate(zip(high, low)):
            a_ref[k, rows, :] = jnp.where(even, h, l)
            c_ref[k, rows, :] = jnp.where(even, l, h)
    for c in planes:
        c.wait()


HBM = pltpu.MemorySpace.HBM
VMEM = pltpu.MemorySpace.VMEM


def pack(noisy, bound):
    ni, nx, nz = noisy.shape
    depth = nz // LANES
    message = pltpu.VMEM((3, ni, nz), F32)
    boundary = pltpu.VMEM((4, nx, nz), F32)
    return pl.pallas_call(
        pack_kernel,
        out_shape=(message, message, boundary, boundary),
        in_specs=[pl.BlockSpec(memory_space=HBM)] * 2,
        out_specs=[pl.BlockSpec(memory_space=VMEM)] * 4,
        scratch_shapes=[
            pltpu.VMEM((4, 2, ni, nz), F32),
            pltpu.SemaphoreType.DMA((4, 2)),
            pltpu.SemaphoreType.DMA((2, 2)),
        ],
        compiler_params=pltpu.CompilerParams(vmem_limit_bytes=8 << 20),
        name="pack_faces",
    )(noisy, bound)


def strip(s):
    return pl.ds(OWN + 8 * s, 8)


def strip_next(s):
    return pl.ds(OWN + 8 * s + 1, 8)


def strip_back(s):
    return pl.ds(OWN + 8 * s - 1, 8)


def wrap_rows(field, p, depth):
    for j in range(depth):
        field[p, j, pl.ds(HALO + 8, 1), :] = field[p, j, pl.ds(OWN, 1), :]


def scale(p, depth, image_of, ve):
    for j in range(depth):
        for s in range(5):
            ve[p, j, strip(s), :] = SIGMA * image_of(p, j, s)
    wrap_rows(ve, p, depth)


def tile(field, p, j, s):
    return field[p, pl.ds(8 * s, 8), pl.ds(j * LANES, LANES)]


def x_dual(p, s, depth, ve, v, b, c):
    return [
        clip2(ve[p, j, strip_next(s), :] - v[j], b[j], c[j]) for j in range(depth)
    ]


def clip2(value, bound, below):
    return jnp.minimum(jnp.maximum(value, below), bound)


ORDER = (4, 0, 1, 2, 3)


def crossline(p, q, depth, ve, bound_of, dx, then):
    for s in (3,) + ORDER:
        v = [ve[p, j, strip(s), :] for j in range(depth)]
        b = [bound_of(p, j, s) for j in range(depth)]
        c = [-k for k in b]
        x = x_dual(p, s, depth, ve, v, b, c)
        for j in range(depth):
            dx[q, j, strip(s), :] = x[j]
        if s == 3:
            break
    for s in ORDER:
        v = [ve[p, j, strip(s), :] for j in range(depth)]
        b = [bound_of(p, j, s) for j in range(depth)]
        c = [-k for k in b]
        if s == 3:
            x = [dx[q, j, strip(s), :] for j in range(depth)]
        else:
            x = x_dual(p, s, depth, ve, v, b, c)
            for j in range(depth):
                dx[q, j, strip(s), :] = x[j]
        z = [clip2(n - o, k, m) for n, o, k, m in zip(depth_next(v), v, b, c)]
        back = depth_back(z)
        div = [x[j] - dx[q, j, strip_back(s), :] + (z[j] - back[j]) for j in range(depth)]
        then(s, v, b, c, x, z, div)
        if s == 4:
            for j in range(depth):
                dx[q, j, pl.ds(OWN - 1, 1), :] = dx[q, j, pl.ds(HALO + 7, 1), :]


def planes_kernel(
    n4_ref, b4_ref, sent_a, sent_c, got_a, got_c, _,
    a_ref, c_ref, hn, hb, ve, dx, far,
):
    ni, depth = got_a.shape[1], got_a.shape[2] // LANES
    _, more_x, even_i, even_x = place()

    for r in range(0, ni, 8):
        rows = pl.ds(r, 8)
        a = [got_a[k, rows, :] for k in range(3)]
        c = [got_c[k, rows, :] for k in range(3)]
        after = [jnp.where(even_x, k, m) for k, m in zip(a, c)]
        before = [jnp.where(even_x, m, k) for k, m in zip(a, c)]
        last = jnp.where(even_x, sent_a[0, rows, :], sent_c[0, rows, :])
        far[0, rows, :] = jnp.where(more_x, after[0], last)
        far[1, rows, :] = after[0] + after[2] * (1.0 / SIGMA)
        far[2, rows, :] = before[0] - before[2] * (1.0 / SIGMA)
        far[3, rows, :] = before[0]
        far[4, rows, :] = after[1]
        far[5, rows, :] = before[1]

    wide = jnp.full((1, LANES), WIDE, F32)

    for i in range(ni):
        for j in range(depth):
            lanes = pl.ds(j * LANES, LANES)
            for k, row in enumerate((0, 1, 6, 7)):
                hn[i, j, row : row + 1, :] = far[k, i : i + 1, lanes]
            hb[i, j, 0:1, :] = far[4, i : i + 1, lanes]
            hb[i, j, 6:7, :] = wide
            hb[i, j, 7:8, :] = far[5, i : i + 1, lanes]
    planes_at = (0, 1, ni - 2, ni - 1)

    def image_of(q, j, s):
        return hn[planes_at[q], j, 0:8, :] if s == 4 else tile(n4_ref, q, j, s)

    def bound_of(q, j, s):
        return hb[planes_at[q], j, 0:8, :] if s == 4 else tile(b4_ref, q, j, s)

    for q in range(4):
        scale(q, depth, image_of, ve)

    def up(ref):
        for s in range(5):
            for j in range(depth):
                ref[j, pl.ds(8 * s, 8), :] = image_of(3, j, s)
                ref[j, pl.ds(40 + 8 * s, 8), :] = bound_of(3, j, s)

        def then(s, v, b, c, x, z, div):
            if s == 4:
                return
            for j in range(depth):
                before = clip(v[j] - ve[2, j, strip(s), :], bound_of(2, j, s))
                ref[j, pl.ds(80 + 8 * s, 8), :] = div[j] - before

        crossline(3, 3, depth, ve, bound_of, dx, then)

    def down(ref):
        for s in range(5):
            for j in range(depth):
                ref[j, pl.ds(8 * s, 8), :] = image_of(0, j, s)

        def then(s, v, b, c, x, z, div):
            if s == 4:
                return
            for j in range(depth):
                own = clip2(ve[1, j, strip(s), :] - v[j], b[j], c[j])
                ref[j, pl.ds(40 + 8 * s, 8), :] = div[j] + own

        crossline(0, 0, depth, ve, bound_of, dx, then)

    @pl.when(even_i)
    def _():
        up(a_ref)
        down(c_ref)

    @pl.when(jnp.logical_not(even_i))
    def _():
        down(a_ref)
        up(c_ref)


def planes(n4, b4, sent_a, sent_c, got_a, got_c, after):
    ni, depth = got_a.shape[1], got_a.shape[2] // LANES
    buffer = pltpu.VMEM((4, depth, ROWS, LANES), F32)
    return pl.pallas_call(
        planes_kernel,
        out_shape=(pltpu.VMEM((depth, 112, LANES), F32),) * 2
        + (pltpu.VMEM((ni, depth, 8, LANES), F32),) * 2,
        in_specs=[pl.BlockSpec(memory_space=VMEM)] * 7,
        out_specs=[pl.BlockSpec(memory_space=VMEM)] * 4,
        scratch_shapes=[buffer] * 2 + [pltpu.VMEM((6, ni, depth * LANES), F32)],
        compiler_params=pltpu.CompilerParams(vmem_limit_bytes=8 << 20),
        name="pack_planes",
    )(n4, b4, sent_a, sent_c, got_a, got_c, after)


class Fields:
    def __init__(self, ring, **fields):
        self.ring = ring
        self.__dict__.update(fields)


class Split:
    def __init__(self, given, own, slots):
        self.given, self.own, self.slots = given, own, slots

    def __getitem__(self, index):
        return (self.given if index[0] in self.slots else self.own)[index]

    def __setitem__(self, index, value):
        self.own[index] = value


def first(t, p, depth, more_x, sums):
    sums = list(sums)
    q, before = t.ring(p), t.ring(p - 1)

    def then(s, v, b, c, x, z, div):
        for j in range(depth):
            i_new = clip2(t.ve[p + 1, j, strip(s), :] - v[j], b[j], c[j])
            t.di[q, j, strip(s), :] = i_new
            total = div[j] + (i_new - t.di[before, j, strip(s), :])
            t.ue[p, j, strip(s), :] = v[j] + TWO_CS * total
            if s < 4:
                t.dz[q, j, strip(s), :] = z[j]
                t.div1[q, j, strip(s), :] = total
                sums[0] = sums[0] + total * total
                sums[1] = sums[1] + (x[j] * x[j] + (i_new * i_new + z[j] * z[j]))

    crossline(p, q, depth, t.ve, t.bound_of, t.dx, then)
    for j in range(depth):
        edge = t.ue[p, j, pl.ds(HALO - 1, 1), :]
        t.ue[p, j, pl.ds(HALO, 1), :] = jnp.where(more_x, t.ue[p, j, pl.ds(HALO, 1), :], edge)
    wrap_rows(t.ue, p, depth)
    return tuple(sums)


def second_i(t, p, s, j):
    q = t.ring(p)
    t.di2[q, j, strip(s), :] = clip(
        t.di_of(p, j, s) + (t.ue[p + 1, j, strip(s), :] - t.ue[p, j, strip(s), :]),
        t.bound_of(p, j, s),
    )


def second(t, p, o, depth, sums, uo, do):
    p2, d2 = sums
    q, before = t.ring(p), t.ring(p - 1)
    for s in ORDER:
        u = [t.ue[p, j, strip(s), :] for j in range(depth)]
        b = [t.bound_of(p, j, s) for j in range(depth)]
        c = [-k for k in b]
        x_old = [t.dx[q, j, strip(s), :] for j in range(depth)]
        x_new = [
            clip2(x_old[j] + (t.ue[p, j, strip_next(s), :] - u[j]), b[j], c[j])
            for j in range(depth)
        ]
        for j in range(depth):
            t.dx2[q, j, strip(s), :] = x_new[j]
        if s == 4:
            for j in range(depth):
                t.dx2[q, j, pl.ds(OWN - 1, 1), :] = t.dx2[q, j, pl.ds(HALO + 7, 1), :]
            continue
        z_old = [t.dz_of(p, j, s) for j in range(depth)]
        z_new = [
            clip2(z_old[j] + (n - u[j]), b[j], c[j]) for j, n in enumerate(depth_next(u))
        ]
        back = depth_back(z_new)
        rows = pl.ds(8 * s, 8)
        for j in range(depth):
            lanes = pl.ds(j * LANES, LANES)
            i_old = t.di_of(p, j, s)
            i_new = clip2(i_old + (t.ue[p + 1, j, strip(s), :] - u[j]), b[j], c[j])
            t.di2[q, j, strip(s), :] = i_new
            total = (
                (x_new[j] - t.dx2[q, j, strip_back(s), :])
                + (z_new[j] - back[j])
                + (i_new - t.di2[before, j, strip(s), :])
            )
            old = t.div1[q, j, strip(s), :]
            uo[o, rows, lanes] = t.image_of(p, j, s) + (C * total + C_OLD * old)
            do[0, o, rows, lanes] = i_new
            do[1, o, rows, lanes] = x_new[j]
            do[2, o, rows, lanes] = z_new[j]
            gap = total - C * old
            p2 = p2 + gap * gap
            gi = i_new - i_old
            gx = x_new[j] - x_old[j]
            gz = z_new[j] - z_old[j]
            d2 = d2 + (gi * gi + (gx * gx + gz * gz))
    return p2, d2


KEPT = {1: 0, 2: 1, 5: 2, 6: 3}


def boundary_planes(ni):
    return 0, 1, ni - 2, ni - 1


GROUP = 3
PART = 2
HANDED = (
    ("ve", (1, 2, 5, 6)),
    ("ue", (2, 3, 4, 5)),
    ("di", (2, 5)),
    ("dx", (2, 5)),
    ("dz", (2, 5)),
    ("div1", (2, 5)),
    ("di2", (4,)),
)


def own_kernel(n_hbm, b_hbm, nv, bv, di, dz, part, sum_ref, sems):
    ni, depth = n_hbm.shape[0], n_hbm.shape[2] // LANES
    steps = (ni - 2) // GROUP

    def reads(c, start, count):
        span = pl.ds(start, count)
        return [
            pltpu.make_async_copy(src.at[span], dst.at[span], sems.at[k, c])
            for k, (src, dst) in enumerate(((n_hbm, nv), (b_hbm, bv)))
        ]

    ahead = reads(0, 0, GROUP + 2)
    for copy in ahead:
        copy.start()
    for c in range(1, steps):
        for copy in reads(c, c * GROUP + 2, GROUP):
            copy.start()
    for copy in ahead:
        copy.wait()

    def spot(j, s):
        return pl.ds(8 * s, 8), pl.ds(j * LANES, LANES)

    for s in range(4):
        for j in range(depth):
            gap = SIGMA * (tile(nv, 1, j, s) - tile(nv, 0, j, s))
            di[(0,) + spot(j, s)] = clip(gap, tile(bv, 0, j, s))

    def body(step, total):
        @pl.when(step > 0)
        def _():
            for copy in reads(step, step * GROUP + 2, GROUP):
                copy.wait()

        for k in range(GROUP):
            p = step * GROUP + 1 + k
            for s in range(4):
                n = [tile(nv, p, j, s) for j in range(depth)]
                b = [tile(bv, p, j, s) for j in range(depth)]
                c = [-k for k in b]
                z = [clip2(SIGMA * (m - o), k, l) for m, o, k, l in zip(depth_next(n), n, b, c)]
                back = depth_back(z)
                for j in range(depth):
                    new = clip2(SIGMA * (tile(nv, p + 1, j, s) - n[j]), b[j], c[j])
                    at = (p,) + spot(j, s)
                    di[at] = new
                    dz[at] = z[j]
                    part[at] = (new - tile(di, p - 1, j, s)) + (z[j] - back[j])
                    total = total + (new * new + z[j] * z[j])
        return total

    sum_ref[0] = lax.fori_loop(0, steps, body, jnp.zeros((8, LANES), F32))


def own(noisy, bound):
    ni, nx, nz = noisy.shape
    whole = pltpu.VMEM((ni, nx, nz), F32)
    return pl.pallas_call(
        own_kernel,
        out_shape=(whole,) * 5 + (pltpu.VMEM((4, 8, LANES), F32),),
        in_specs=[pl.BlockSpec(memory_space=HBM)] * 2,
        out_specs=[pl.BlockSpec(memory_space=VMEM)] * 6,
        scratch_shapes=[pltpu.SemaphoreType.DMA((2, (ni - 2) // GROUP))],
        compiler_params=pltpu.CompilerParams(vmem_limit_bytes=16 << 20),
        cost_estimate=pl.CostEstimate(flops=100_000_000, transcendentals=0, bytes_accessed=4 << 20),
        name="own_planes",
    )(noisy, bound)


def inner_kernel(nv, bv, di, dz, part, own_sum, hn, hb, u_hbm, d_hbm, sums_ref, *refs):
    handed, refs = refs[: len(HANDED)], refs[len(HANDED) :]
    ve, ue, dh, dx, div1, dx2, di2, uo, do, u_sems, d_sems = refs
    ni, depth = nv.shape[0], nv.shape[2] // LANES
    more_x = place()[1]
    parts = (ni - 4) // PART

    def bound_of(p, j, s):
        return hb[p, j, 0:8, :] if s == 4 else tile(bv, p, j, s)

    def image_of(p, j, s):
        return hn[p, j, 0:8, :] if s == 4 else tile(nv, p, j, s)

    def di_of(p, j, s):
        return dh[p % 4, j, 0:8, :] if s == 4 else tile(di, p, j, s)

    t = Fields(
        lambda p: p % 4,
        bound_of=bound_of, image_of=image_of, di_of=di_of,
        dz_of=lambda p, j, s: tile(dz, p, j, s),
        ve=ve, ue=ue, dx=dx, div1=div1, dx2=dx2, di2=di2,
    )

    def writes(c):
        span = pl.ds(c * PART + 2, PART)
        return [pltpu.make_async_copy(uo.at[span], u_hbm.at[span], u_sems.at[c])] + [
            pltpu.make_async_copy(do.at[k, span], d_hbm.at[k, span], d_sems.at[k, c])
            for k in range(3)
        ]

    def hand(slots):
        for ref, (name, wanted) in zip(handed, HANDED):
            for slot in wanted:
                if slot not in slots:
                    continue
                plane = slot - 1 if slot < 4 else ni - 7 + slot
                for j in range(depth):
                    for s in range(4 if name in ("dz", "div1", "di2") else 5):
                        if name == "di":
                            value = di_of(plane, j, s)
                        elif name == "dz":
                            value = tile(dz, plane, j, s)
                        elif name in ("ve", "ue"):
                            value = getattr(t, name)[plane, j, strip(s), :]
                        else:
                            value = getattr(t, name)[plane % 4, j, strip(s), :]
                        ref[slot, j, strip(s), :] = value
                    if name in ("ve", "ue"):
                        behind = pl.ds(HALO + 8, 1)
                        ref[slot, j, behind, :] = getattr(t, name)[plane, j, behind, :]

    def ready(p):
        scale(p, depth, image_of, ve)

    def halo_i(p):
        return [
            clip(ve[p + 1, j, strip(4), :] - ve[p, j, strip(4), :], hb[p, j, 0:8, :])
            for j in range(depth)
        ]

    def first_inner(p, sums):
        p1, d1 = sums
        q = p % 4
        for s in (3,) + ORDER[:4]:
            v = [ve[p, j, strip(s), :] for j in range(depth)]
            b = [bound_of(p, j, s) for j in range(depth)]
            c = [-k for k in b]
            x = x_dual(p, s, depth, ve, v, b, c)
            for j in range(depth):
                dx[q, j, strip(s), :] = x[j]
            if s == 3:
                continue
            finish = [x[j] - dx[q, j, strip_back(s), :] for j in range(depth)]
            if s == 4:
                z = [clip2(n - o, k, m) for n, o, k, m in zip(depth_next(v), v, b, c)]
                back = depth_back(z)
                new = halo_i(p)
                for j in range(depth):
                    below = new[j] - dh[(p - 1) % 4, j, 0:8, :]
                    dh[q, j, 0:8, :] = new[j]
                    total = finish[j] + (z[j] - back[j]) + below
                    ue[p, j, strip(4), :] = v[j] + TWO_CS * total
                    dx[q, j, pl.ds(OWN - 1, 1), :] = dx[q, j, pl.ds(HALO + 7, 1), :]
                continue
            for j in range(depth):
                total = finish[j] + tile(part, p, j, s)
                ue[p, j, strip(s), :] = v[j] + TWO_CS * total
                div1[q, j, strip(s), :] = total
                p1 = p1 + total * total
                d1 = d1 + x[j] * x[j]
        s = 3
        for j in range(depth):
            x3 = dx[q, j, strip(s), :]
            total = (x3 - dx[q, j, strip_back(s), :]) + tile(part, p, j, s)
            ue[p, j, strip(s), :] = ve[p, j, strip(s), :] + TWO_CS * total
            div1[q, j, strip(s), :] = total
            p1 = p1 + total * total
            d1 = d1 + x3 * x3
        for j in range(depth):
            edge = ue[p, j, pl.ds(HALO - 1, 1), :]
            ue[p, j, pl.ds(HALO, 1), :] = jnp.where(more_x, ue[p, j, pl.ds(HALO, 1), :], edge)
        wrap_rows(ue, p, depth)
        return p1, d1

    for p in range(4):
        ready(p)
    for j, value in enumerate(halo_i(0)):
        dh[0, j, 0:8, :] = value
    zero = jnp.zeros((8, LANES), F32)
    a = first_inner(1, (zero, own_sum[0]))
    a = first_inner(2, a)
    for s in range(4):
        for j in range(depth):
            second_i(t, 1, s, j)
    hand((1, 2, 3))

    def body(step, carry):
        a, b = carry
        for k in range(PART):
            p = step * PART + 3 + k
            ready(p + 1)
            a = first_inner(p, a)
            b = second(t, p - 1, p - 1, depth, b, uo, do)
        for copy in writes(step):
            copy.start()
        return a, b

    a, b = lax.fori_loop(0, parts, body, (a, (zero, zero)))
    hand((4, 5, 6))
    for k, total in enumerate(a + b):
        sums_ref[k] = total
    for c in range(parts):
        for copy in writes(c):
            copy.wait()


def inner(nv, bv, di, dz, part, own_sum, halo_n, halo_b):
    ni, nx, nz = nv.shape
    depth = nz // LANES
    full = pltpu.VMEM((ni, depth, ROWS, LANES), F32)
    short = pltpu.VMEM((4, depth, ROWS, LANES), F32)
    parts = (ni - 4) // PART
    slots = pltpu.VMEM((8, depth, ROWS, LANES), F32)
    return pl.pallas_call(
        inner_kernel,
        out_shape=(
            jax.ShapeDtypeStruct((ni, nx, nz), F32),
            jax.ShapeDtypeStruct((3, ni, nx, nz), F32),
            pltpu.VMEM((4, 8, LANES), F32),
        )
        + (slots,) * len(HANDED),
        in_specs=[pl.BlockSpec(memory_space=VMEM)] * 8,
        out_specs=[pl.BlockSpec(memory_space=HBM)] * 2
        + [pl.BlockSpec(memory_space=VMEM)] * (1 + len(HANDED)),
        scratch_shapes=[full] * 2
        + [pltpu.VMEM((4, depth, 8, LANES), F32)]
        + [short] * 4
        + [
            pltpu.VMEM((ni, nx, nz), F32),
            pltpu.VMEM((3, ni, nx, nz), F32),
            pltpu.SemaphoreType.DMA((parts,)),
            pltpu.SemaphoreType.DMA((3, parts)),
        ],
        compiler_params=pltpu.CompilerParams(vmem_limit_bytes=24 << 20),
        cost_estimate=pl.CostEstimate(flops=200_000_000, transcendentals=0, bytes_accessed=12 << 20),
        name="inner_planes",
    )(nv, bv, di, dz, part, own_sum, halo_n, halo_b)


def edge_kernel(got_a, got_c, n4_ref, b4_ref, hb, sums_ref, *refs):
    given = dict(zip([name for name, _ in HANDED], refs))
    refs = refs[len(HANDED) :]
    _, _, u_hbm, d_hbm, spread_ref = refs[:5]
    ve, ue, di, dx, dz, div1, di2, dx2, uo, do, u_sems, d_sems = refs[5:]
    own = dict(ve=ve, ue=ue, di=di, dx=dx, dz=dz, div1=div1, di2=di2)
    depth, ni = got_a.shape[0], u_hbm.shape[0]
    more_i, more_x, even_i, _ = place()

    def up(j, row):
        rows = pl.ds(row, 8)
        return jnp.where(even_i, got_c[j, rows, :], got_a[j, rows, :])

    def down(j, row):
        rows = pl.ds(row, 8)
        return jnp.where(even_i, got_a[j, rows, :], got_c[j, rows, :])

    def bound_of(p, j, s):
        if p == 0:
            return up(j, 40 + 8 * s)
        return hb[boundary_planes(ni)[KEPT[p]], j, 0:8, :] if s == 4 else tile(b4_ref, KEPT[p], j, s)

    t = Fields(
        lambda p: p,
        dx2=dx2,
        bound_of=bound_of,
        image_of=lambda p, j, s: tile(n4_ref, KEPT[p], j, s),
        di_of=lambda p, j, s: t.di[p, j, strip(s), :],
        dz_of=lambda p, j, s: t.dz[p, j, strip(s), :],
        **{name: Split(given[name], own[name], slots) for name, slots in HANDED},
    )
    a = sums_ref[0], sums_ref[1]
    b = sums_ref[2], sums_ref[3]

    for j in range(depth):
        for s in range(5):
            t.ve[0, j, strip(s), :] = SIGMA * up(j, 8 * s)
            t.ve[7, j, strip(s), :] = jnp.where(
                more_i, SIGMA * down(j, 8 * s), t.ve[6, j, strip(s), :]
            )
    for j in range(depth):
        for s in range(5):
            low = clip(t.ve[1, j, strip(s), :] - t.ve[0, j, strip(s), :], up(j, 40 + 8 * s))
            t.di[0, j, strip(s), :] = low
            if s < 4:
                part = up(j, 80 + 8 * s)
                t.ue[0, j, strip(s), :] = t.ve[0, j, strip(s), :] + TWO_CS * (part + low)
    a = first(t, 1, depth, more_x, a)
    for s in range(4):
        for j in range(depth):
            second_i(t, 0, s, j)
    b = second(t, 1, 0, depth, b, uo, do)
    b = second(t, 2, 1, depth, b, uo, do)

    def writes(k, plane):
        at, to = pl.ds(2 * k, 2), pl.ds(plane, 2)
        return [pltpu.make_async_copy(uo.at[at], u_hbm.at[to], u_sems.at[k])] + [
            pltpu.make_async_copy(do.at[c, at], d_hbm.at[c, to], d_sems.at[c, k]) for c in range(3)
        ]

    copies = writes(0, 0)
    for copy in copies:
        copy.start()
    a = first(t, 6, depth, more_x, a)
    for j in range(depth):
        for s in range(4):
            part = down(j, 40 + 8 * s)
            top = t.ve[7, j, strip(s), :] + TWO_CS * (part - t.di[6, j, strip(s), :])
            t.ue[7, j, strip(s), :] = jnp.where(more_i, top, t.ue[6, j, strip(s), :])
    b = second(t, 5, 2, depth, b, uo, do)
    b = second(t, 6, 3, depth, b, uo, do)
    last = writes(1, ni - 2)
    for copy in last:
        copy.start()
    factors = (C * C, 1.0, C * C, 1.0)
    lane = lax.broadcasted_iota(jnp.int32, (1, 4), 1)
    row = jnp.zeros((1, 4), F32)
    for k, total in enumerate(a + b):
        row = jnp.where(lane == k, factors[k] * jnp.sum(total), row)
    spread_ref[...] = jnp.broadcast_to(row, spread_ref.shape)
    for copy in copies + last:
        copy.wait()


def edges(got_a, got_c, n4, b4, halo_b, sums, handed, primal, dual, devices):
    _, nx, nz = primal.shape
    depth = nz // LANES
    buffer = pltpu.VMEM((8, depth, ROWS, LANES), F32)
    count = 6 + len(handed)
    return pl.pallas_call(
        edge_kernel,
        out_shape=(
            jax.ShapeDtypeStruct(primal.shape, F32),
            jax.ShapeDtypeStruct(dual.shape, F32),
            jax.ShapeDtypeStruct((devices, 4), F32),
        ),
        in_specs=[pl.BlockSpec(memory_space=VMEM)] * count
        + [pl.BlockSpec(memory_space=HBM)] * 2,
        out_specs=[pl.BlockSpec(memory_space=HBM)] * 2 + [pl.BlockSpec(memory_space=VMEM)],
        scratch_shapes=[buffer] * 8
        + [
            pltpu.VMEM((4, nx, nz), F32),
            pltpu.VMEM((3, 4, nx, nz), F32),
            pltpu.SemaphoreType.DMA((2,)),
            pltpu.SemaphoreType.DMA((3, 2)),
        ],
        input_output_aliases={count: 0, count + 1: 1},
        compiler_params=pltpu.CompilerParams(vmem_limit_bytes=24 << 20),
        name="edge_planes",
    )(got_a, got_c, n4, b4, halo_b, sums, *handed, primal, dual)


def per_device(noisy, bound):
    count_i, count_x = lax.axis_size("inl"), lax.axis_size("xln")
    noisy, bound = (pltpu.with_memory_space_constraint(x, HBM) for x in (noisy, bound))
    send_a, send_c, n4, b4 = pack(noisy, bound)
    got_c = swapped(send_c, "xln", 1)
    got_a = swapped(send_a, "xln", 0)
    alone = own(noisy, bound)
    face_a, face_c, halo_n, halo_b = planes(
        n4, b4, send_a, send_c, got_a, got_c, alone[-1]
    )
    back_a = swapped(face_a, "inl", 0)
    back_c = swapped(face_c, "inl", 1)
    primal, dual, sums, *handed = inner(*alone, halo_n, halo_b)
    primal, dual, spread = edges(
        back_a, back_c, n4, b4, halo_b, sums, handed, primal, dual, count_i * count_x
    )
    parts = lax.all_to_all(spread, AXES, 0, 0, tiled=True)
    norms = jnp.sqrt(jnp.sum(parts, axis=0)).reshape(2, 2)
    return primal, dual, norms


def solution(mesh):
    in_specs = (P("inl", "xln", None), P("inl", "xln", None))
    out_specs = (P("inl", "xln", None), P(None, "inl", "xln", None), P())
    return jax.shard_map(
        per_device, mesh=mesh, in_specs=in_specs, out_specs=out_specs, check_vma=False
    )
```
